32 devices in a mesh: gy: 8 (over z, y), gz: 4 (over x, core).
Axes of the slice: x: 2, y: 2, z: 4, core: 2. Of those that a mesh axis runs over, the one named last changes fastest.
Arguments:
- tokens: bfloat16 [2, 64, 8, 8, 1024], P(None, None, 'gy', 'gz'), may hold values from -64 to 64
- w_qkv: bfloat16 [1024, 3072], P('gy'), may hold values from -2 to 2
- w_out: bfloat16 [1024, 1024], P('gy'), may hold values from -0.1875 to 0.1875
- bias_x: float32 [16, 127], replicated, may hold values from -4 to 4
- bias_y: float32 [16, 15], replicated, may hold values from -4 to 4
- bias_z: float32 [16, 15], replicated, may hold values from -4 to 4
Outputs:
- mixed: bfloat16 [2, 64, 8, 8, 1024], P(None, None, 'gy', 'gz')
The draws below stay inside these ranges and needn't reach their ends.
All inputs are finite; a program needn't handle non-finite values.
Results may differ from the reference program's by a relative error of at most 0.0083.
Values may be sent and summed in bfloat16 or wider, within the bound.
A program may use at most 64 MiB of HBM per device.

```python
import math
import jax
import jax.numpy as jnp
from jax import lax

D = 1024
HEADS = 16
HEAD = 64
SAMPLES = 2
NX = 64
NY = 8
NZ = 8


def draw_tokens(key, part):
    streams = jax.random.split(jax.random.fold_in(key, 11), 1)
    dims = (SAMPLES, NX, NY, NZ, D)
    values = jax.random.normal(streams[0], dims, jnp.float32)
    values = values * 0.25
    return jnp.clip(values, -64.0, 64.0).astype(jnp.bfloat16)


def draw_w_qkv(key, part):
    limit = 6.0 / math.sqrt(D)
    base = jax.random.normal(jax.random.fold_in(key, 12), (D, 3 * D), jnp.float32) / math.sqrt(D)
    base = jnp.clip(base, -limit, limit)
    return jnp.clip(base, -2.0, 2.0).astype(jnp.bfloat16)


def levels(stream_key, extent, cuts, smallest, top_value):
    gain, own = 1.0, jax.random.fold_in(stream_key, 6)
    for position, blocks in cuts:
        steps = jnp.exp(jax.random.uniform(jax.random.fold_in(own, position), (blocks,), jnp.float32, smallest / len(cuts), top_value / len(cuts)))
        gain = gain * jnp.repeat(steps, extent[position] // blocks).reshape([-1 if axis == position else 1 for axis in range(len(extent))])
    return gain


def normal_values(own_key, extent, scale, most, cuts=(), held_as=jnp.bfloat16):
    values = jax.random.normal(own_key, extent, jnp.float32) * scale
    if len(cuts) > 0:
        values = levels(own_key, extent, cuts, -0.22, 0.18) * values
    return jnp.clip(values, min=-most, max=most).astype(held_as)


def setup_inputs(seed: int = 0) -> dict:
    splits = jax.random.split(jax.random.key(seed), 7)
    return {
        "tokens": draw_tokens(jax.random.fold_in(splits[6], 71), 0),
        "w_qkv": draw_w_qkv(jax.random.fold_in(splits[6], 71), 0),
        "w_out": normal_values(splits[2], (D, D), D ** -0.5, 0.1875, ((0, 8),)),
        "bias_x": normal_values(splits[3], (HEADS, 2 * NX - 1), 1.0, 4.0, (), jnp.float32),
        "bias_y": normal_values(splits[4], (HEADS, 2 * NY - 1), 1.0, 4.0, (), jnp.float32),
        "bias_z": normal_values(splits[5], (HEADS, 2 * NZ - 1), 1.0, 4.0, (), jnp.float32),
    }


einsum_forms = {1: ('bxyzhs,bwyzhs->byzhxw', 'byzhxw,bwyzhs->bxyzhs'), 2: ('bxyzhs,bxwzhs->bxzhyw', 'bxzhyw,bxwzhs->bxyzhs'), 3: ('bxyzhs,bxywhs->bxyhzw', 'bxyhzw,bxywhs->bxyzhs')}

def norm_rows(tokens):
    values = tokens.astype(jnp.float32)
    center = lax.optimization_barrier(jnp.mean(values, axis=-1, keepdims=True))
    spread = lax.optimization_barrier(jnp.mean((values - center) ** 2, axis=-1, keepdims=True))
    return ((values - center) * lax.rsqrt(spread + 1e-05)).astype(jnp.bfloat16)

def rel_bias(table):
    length = (table.shape[1] + 1) // 2
    offsets = jnp.arange(length)[:, None] - jnp.arange(length)[None, :] + length - 1
    return table[:, offsets.astype(jnp.int32)]

def attend(qkv, table, axis):
    dims = qkv.shape
    features = dims[-1] // 3
    parts = qkv.reshape(dims[:-1] + (3, HEADS, HEAD))
    query = parts[..., 0, :, :].astype(jnp.float32)
    keys = parts[..., 1, :, :].astype(jnp.float32)
    values = parts[..., 2, :, :].astype(jnp.float32)
    score_form, mix_form = einsum_forms[axis]
    scores = jnp.einsum(score_form, query, keys) * HEAD ** (-0.5) + rel_bias(table)
    scores = scores - lax.optimization_barrier(jnp.max(scores, axis=-1, keepdims=True))
    expo = jnp.exp(scores)
    weights = (expo / lax.optimization_barrier(jnp.sum(expo, axis=-1, keepdims=True))).astype(jnp.bfloat16)
    mixed = jnp.einsum(mix_form, weights.astype(jnp.float32), values)
    return mixed.reshape(dims[:-1] + (features,)).astype(jnp.bfloat16)

def reference(tokens, w_qkv, w_out, bias_x, bias_y, bias_z):

    def one_sample(sample):
        normed = norm_rows(sample)
        qkv = jnp.dot(normed.reshape(-1, D), w_qkv, preferred_element_type=jnp.float32)
        qkv = qkv.astype(jnp.bfloat16).reshape((1, NX, NY, NZ, 3 * D))
        along_x = attend(qkv, bias_x, 1).astype(jnp.float32)
        along_y = attend(qkv, bias_y, 2).astype(jnp.float32)
        along_z = attend(qkv, bias_z, 3).astype(jnp.float32)
        summed = (along_x + along_y + along_z).astype(jnp.bfloat16).reshape(-1, D)
        result = jnp.dot(summed, w_out, preferred_element_type=jnp.float32)
        result = result + sample.reshape(-1, D).astype(jnp.float32)
        return result.astype(jnp.bfloat16).reshape((NX, NY, NZ, D))
    return lax.map(one_sample, tokens)
```

```python
import functools

import jax
import jax.numpy as jnp
import numpy as np
from jax import lax
from jax.experimental import pallas as pl
from jax.experimental.pallas import tpu as pltpu
from jax.sharding import PartitionSpec as P

HEADS = 16
HEAD = 64


einsum_forms = {
    1: ("bxyzhs,bwyzhs->byzhxw", "byzhxw,bwyzhs->bxyzhs"),
    2: ("bxyzhs,bxwzhs->bxzhyw", "bxzhyw,bxwzhs->bxyzhs"),
    3: ("bxyzhs,bxywhs->bxyhzw", "bxyhzw,bxywhs->bxyzhs"),
}


def norm_rows(tokens):
    values = tokens.astype(jnp.float32)
    center = jnp.mean(values, axis=-1, keepdims=True)
    spread = jnp.mean((values - center) ** 2, axis=-1, keepdims=True)
    return ((values - center) * lax.rsqrt(spread + 1e-05)).astype(jnp.bfloat16)


def rel_bias(table):
    length = (table.shape[1] + 1) // 2
    offsets = (
        lax.broadcasted_iota(jnp.int32, (length, length), 0)
        - lax.broadcasted_iota(jnp.int32, (length, length), 1)
        + length
        - 1
    )
    lookup = (
        offsets[:, :, None] == lax.broadcasted_iota(jnp.int32, (1, 1, 2 * length - 1), 2)
    ).astype(jnp.float32)
    return jnp.einsum("hr,ijr->hij", table, lookup, precision=lax.Precision.HIGHEST)


def attend(qkv, table, axis):
    dims = qkv.shape
    features = dims[-1] // 3
    parts = qkv.reshape(dims[:-1] + (3, HEADS, HEAD))
    query = parts[..., 0, :, :]
    keys = parts[..., 1, :, :]
    values = parts[..., 2, :, :]
    score_form, mix_form = einsum_forms[axis]
    scores = jnp.einsum(score_form, query, keys, preferred_element_type=jnp.float32) * HEAD ** (
        -0.5
    ) + rel_bias(table)
    scores = scores - jnp.max(scores, axis=-1, keepdims=True)
    expo = jnp.exp(scores)
    weights = (expo / jnp.sum(expo, axis=-1, keepdims=True)).astype(jnp.bfloat16)
    mixed = jnp.einsum(mix_form, weights, values, preferred_element_type=jnp.float32)
    return mixed.reshape(dims[:-1] + (features,)).astype(jnp.bfloat16)


def return_y(result):
    return lax.all_to_all(result, "gy", split_axis=2, concat_axis=1, tiled=True)


def return_z(result):
    return lax.all_to_all(result, "gz", split_axis=3, concat_axis=1, tiled=True)


def shards(tokens, w_qkv, w_out, bias_x, bias_y, bias_z):
    samples, depth, rows_y, rows_z, features = tokens.shape
    normed = norm_rows(tokens)
    gathered = lax.all_gather(w_qkv, "gy", axis=0, tiled=True)

    def project(inputs):
        product = jnp.dot(
            inputs.reshape(-1, features), gathered, preferred_element_type=jnp.float32
        )
        return product.astype(jnp.bfloat16).reshape(inputs.shape[:-1] + (3 * features,))

    along_x = attend(project(normed), bias_x, 1)
    along_y = return_y(
        attend(
            project(lax.all_to_all(normed, "gy", split_axis=1, concat_axis=2, tiled=True)),
            bias_y,
            2,
        )
    )
    along_z = return_z(
        attend(
            project(lax.all_to_all(normed, "gz", split_axis=1, concat_axis=3, tiled=True)),
            bias_z,
            3,
        )
    )
    summed = along_x.astype(jnp.float32) + along_y.astype(jnp.float32) + along_z.astype(jnp.float32)
    summed = summed.astype(jnp.bfloat16).reshape(-1, features)
    residual = tokens.reshape(-1, features).astype(jnp.float32)
    result = residual + jnp.dot(
        summed, lax.all_gather(w_out, "gy", axis=0, tiled=True), preferred_element_type=jnp.float32
    )
    return result.astype(jnp.bfloat16).reshape(tokens.shape)


def device(**where):
    return {"device_id": where, "device_id_type": pl.DeviceIdType.MESH}


def line_places(rows, size_y, size_z, rows_z):
    row = np.arange(rows)
    part_y, part_z = rows // size_y, rows // size_z
    return (
        (row // rows_z, row % rows_z),
        (row // part_y, row % part_y),
        (row // part_z * rows_z + row % rows_z, row % part_z // rows_z),
    )


def offset_lookup(places, lengths, rows, width):
    lookup = np.zeros((len(lengths), width, 2 * rows), np.float32)
    for axis, ((position, line), length) in enumerate(zip(places, lengths)):
        first, second = np.nonzero(line[:, None] == line[None, :])
        entry = position[first] - position[second] + length - 1
        lookup[axis, entry, rows - 1 - first + second] = 1.0
    return lookup


def remote(source, target, sends, recvs, **where):
    return pltpu.make_async_remote_copy(
        src_ref=source, dst_ref=target, send_sem=sends, recv_sem=recvs, **device(**where)
    )


def heads_kernel(
    size_y, size_z, rows_z, tokens, w_qkv, w_out, bias_x, bias_y, bias_z, lookup, result,
    lines, wq, wo, padded, offsets, biases, qkv, mixed, ymixed, back, summed, parts, total,
    up_send, up_recv, down_send, down_recv, side_send, side_recv,
    y_send, y_recv, far_send, far_recv, twin_send, twin_recv, relay_send, relay_recv,
    o_send, o_recv, ry_send, ry_recv, ez_send, ez_recv,
):
    me_y, me_z = lax.axis_index("gy"), lax.axis_index("gz")
    samples, rows, features = tokens.shape
    depth = w_qkv.shape[0]
    wide = 2 * HEAD
    pairs = HEADS // (2 * size_z)
    slots = 3 * pairs
    items = slots + pairs
    levels = size_y // 2
    part_y, part_z = rows // size_y, rows // size_z
    level, side = me_y // 2, lax.rem(me_y, 2)
    core, flank = lax.rem(me_z, 2), me_z // 2
    above, below = {"gy": me_y + 2}, {"gy": me_y - 2}
    beside = {"gy": level * 2 + 1 - side}
    twin = me_z + 1 - 2 * core
    far = me_z + 2 - 4 * flank

    barrier = pltpu.get_barrier_semaphore()
    for step in range(1, size_y):
        pl.semaphore_signal(barrier, inc=1, **device(gy=lax.rem(me_y + step, size_y)))
    for step in range(1, size_z):
        pl.semaphore_signal(barrier, inc=1, **device(gz=lax.rem(me_z + step, size_z)))

    values = tokens[...].astype(jnp.float32)
    center = jnp.mean(values, axis=-1, keepdims=True)
    spread = jnp.mean((values - center) ** 2, axis=-1, keepdims=True)
    lines[0, me_z] = ((values - center) * lax.rsqrt(spread + 1e-05)).astype(jnp.bfloat16)

    pl.semaphore_wait(barrier, size_y + size_z - 2)

    def item_ref(item):
        return wq.at[item] if item < slots else wo.at[me_z * pairs + item - slots]

    def own_ref(item):
        if item < slots:
            start = item % 3 * features + (me_z * pairs + item // 3) * wide
            return w_qkv.at[:, pl.ds(pl.multiple_of(start, wide), wide)]
        start = (me_z * pairs + item - slots) * wide
        return w_out.at[:, pl.ds(pl.multiple_of(start, wide), wide)]

    def transfer(item, lev, sid, sends, recvs, slot, where, own=False):
        block = item_ref(item).at[pl.ds(pl.multiple_of((lev * 2 + sid) * depth, depth), depth)]
        source = own_ref(item) if own else block
        return remote(source, block, sends.at[item, slot], recvs.at[item, slot], **where)

    def up(item, step, own=False):
        return transfer(item, level - step, side, up_send, up_recv, step, above, own)

    def up_in(item, step):
        return transfer(item, level - 1 - step, side, up_send, up_recv, step, above)

    def down(item, step, own=False):
        return transfer(item, level + step, side, down_send, down_recv, step, below, own)

    def down_in(item, step):
        return transfer(item, level + 1 + step, side, down_send, down_recv, step, below)

    def across(item, lev, own=False):
        return transfer(item, lev, side, side_send, side_recv, lev, beside, own)

    def across_in(item, lev):
        return transfer(item, lev, 1 - side, side_send, side_recv, lev, beside)

    def own_blocks(item):
        pl.when(level + 1 < levels)(lambda: up(item, 0, True).start())
        pl.when(level > 0)(lambda: down(item, 0, True).start())
        across(item, level, True).start()

    def chain(item, step):
        @pl.when(level - 1 - step >= 0)
        def _():
            up_in(item, step).wait_recv()
            pl.when(level + 1 < levels)(lambda: up(item, step + 1).start())
            across(item, level - 1 - step).start()

        @pl.when(level + 1 + step < levels)
        def _():
            down_in(item, step).wait_recv()
            pl.when(level > 0)(lambda: down(item, step + 1).start())
            across(item, level + 1 + step).start()

    def chains(first, last):
        hops = levels - 1
        for wave in range(first, last + hops - 1):
            for step in range(hops):
                if first <= wave - step < last:
                    chain(wave - step, step)

    def from_side(item):
        for lev in range(levels):
            across_in(item, lev).wait_recv()

    def drain(item):
        pl.when(level + 1 < levels)(lambda: up(item, 0, True).wait_send())
        pl.when(level > 0)(lambda: down(item, 0, True).wait_send())
        across(item, level, True).wait_send()
        for step in range(1, levels):

            @pl.when(level - step >= 0)
            def _():
                pl.when(level + 1 < levels)(lambda: up(item, step).wait_send())
                across(item, level - step).wait_send()

            @pl.when(level + step < levels)
            def _():
                pl.when(level > 0)(lambda: down(item, step).wait_send())
                across(item, level + step).wait_send()

    pieces = samples + size_y

    def piece_of(index, block):
        if index < samples:
            return lines.at[0, block, index]
        peer = lax.rem(me_y + size_y - (index - samples), size_y)
        return lines.at[1, block, :, pl.ds(pl.multiple_of(peer * part_y, part_y), part_y), :]

    def to_far(index, block=me_z):
        ref = piece_of(index, block)
        return remote(ref, ref, far_send.at[index], far_recv.at[index], gz=far)

    def to_twin(index, block=me_z):
        ref = piece_of(index, block)
        return remote(ref, ref, twin_send.at[index], twin_recv.at[index], gz=twin)

    def relay(index, block=far):
        ref = piece_of(index, block)
        return remote(ref, ref, relay_send.at[index], relay_recv.at[index], gz=twin)

    def spread_piece(index):
        to_far(index).start()
        to_twin(index).start()

    def pass_on(index):
        to_far(index, far).wait_recv()
        relay(index).start()

    def exchange(step):
        peer = lax.rem(me_y + step, size_y)
        return remote(
            lines.at[0, me_z, :, pl.ds(pl.multiple_of(peer * part_y, part_y), part_y), :],
            lines.at[1, me_z, :, pl.ds(pl.multiple_of(me_y * part_y, part_y), part_y), :],
            y_send.at[step - 1], y_recv.at[step - 1], gy=peer,
        )

    def exchange_in(step):
        exchange(step).wait_recv()
        spread_piece(samples + step)

    def share_out(slot, block, where):
        ref = wo.at[pl.ds(block * pairs, pairs)]
        return remote(ref, ref, o_send.at[slot], o_recv.at[slot], gz=where)

    def returns(pair):
        copies = []
        for step in range(1, size_y):
            peer = lax.rem(me_y + step, size_y)
            copies.append(
                remote(
                    ymixed.at[pair, peer], back.at[pair, me_y],
                    ry_send.at[pair, step - 1], ry_recv.at[pair, step - 1], gy=peer,
                )
            )
        return copies

    def sums_out(pair):
        copies = []
        for step in range(1, size_z):
            peer = lax.rem(me_z + step, size_z)
            copies.append(
                remote(
                    summed.at[pair, peer], parts.at[pair, me_z],
                    ez_send.at[pair, step - 1], ez_recv.at[pair, step - 1], gz=peer,
                )
            )
        return copies

    row = lax.broadcasted_iota(jnp.int32, (rows, rows), 0)
    col = lax.broadcasted_iota(jnp.int32, (rows, rows), 1)
    lane = lax.broadcasted_iota(jnp.int32, (rows, wide), 1)
    line_of = (
        lambda r: lax.rem(r, rows_z),
        lambda r: lax.rem(r, part_y),
        lambda r: lax.rem(r, part_z) // rows_z,
    )

    def own_weights():
        mine = pl.ds(pl.multiple_of(me_y * depth, depth), depth)
        for item in range(items):
            item_ref(item)[mine, :] = own_ref(item)[...]

    def bias_tables():
        padded[...] = jnp.zeros(padded.shape, jnp.float32)
        for axis, table in enumerate((bias_x, bias_y, bias_z)):
            padded[axis, :, : table.shape[1]] = table[...]
            offsets[axis] = jnp.dot(
                padded[axis], lookup[axis],
                precision=lax.Precision.HIGHEST, preferred_element_type=jnp.float32,
            )

        def fill(head, carry):
            for axis in range(3):
                same = line_of[axis](row) == line_of[axis](col)
                entry = offsets[axis, pl.ds(me_z * 2 * pairs + head, 1), :]
                table = jnp.broadcast_to(entry, (rows, 2 * rows))
                table = pltpu.roll(table, rows + 1, 1, stride=1, stride_axis=0)
                biases[axis, head] = jnp.where(same, table[:, :rows], -1e30)
            return carry

        lax.fori_loop(0, 2 * pairs, fill, 0)

    def project(group, chunk, where):
        blocks = pl.ds(pl.multiple_of(where * 2, 2), 2)
        flat = lines[group, blocks].reshape(2 * samples * rows, features)
        both = jnp.concatenate([wq[2 * chunk], wq[2 * chunk + 1]], axis=1)
        product = jnp.dot(flat, both, preferred_element_type=jnp.float32)
        for half in range(2):
            item = 2 * chunk + half
            piece = product[:, half * wide : (half + 1) * wide]
            if item % 3 == 0:
                piece = piece * HEAD ** (-0.5)
            qkv[group, item, blocks] = piece.astype(jnp.bfloat16).reshape(2, samples, rows, wide)

    def attend(axis, pair, blocks):
        units = [(block, odd) for block in range(len(blocks)) for odd in range(2)]
        scores, expos, totals, outs = {}, {}, {}, {}
        for unit in units:
            block, odd = unit
            query, keys, _ = blocks[block]
            chosen = jnp.where(lane // HEAD == odd, query, 0)
            scores[unit] = lax.dot_general(
                chosen, keys, (((1,), (1,)), ((), ())), preferred_element_type=jnp.float32
            ) + biases[axis, pair * 2 + odd]
        for unit in units:
            expos[unit] = jnp.exp(scores[unit] - jnp.max(scores[unit], axis=-1, keepdims=True))
            totals[unit] = jnp.sum(expos[unit], axis=-1, keepdims=True)
        for unit in units:
            outs[unit] = jnp.dot(
                expos[unit].astype(jnp.bfloat16), blocks[unit[0]][2],
                preferred_element_type=jnp.float32,
            )
        return [
            jnp.where(
                lane < HEAD,
                outs[block, 0] * (1.0 / totals[block, 0]),
                outs[block, 1] * (1.0 / totals[block, 1]),
            ).astype(jnp.bfloat16)
            for block in range(len(blocks))
        ]

    def along_x(pair):
        def body(block, carry):
            blocks = [
                [qkv[0, pair * 3 + m, block, sample] for m in range(3)] for sample in range(samples)
            ]
            for sample, out in enumerate(attend(0, pair, blocks)):
                mixed[0, pair, block, sample] = out
            return carry

        lax.fori_loop(0, size_z, body, 0)

    def along_z(pair):
        def body(index, carry):
            some = pl.ds(pl.multiple_of(index * part_z, part_z), part_z)
            blocks = [
                [
                    jnp.concatenate(
                        [qkv[0, pair * 3 + m, z, sample, some, :] for z in range(size_z)], axis=0
                    )
                    for m in range(3)
                ]
                for sample in range(samples)
            ]
            for sample, out in enumerate(attend(2, pair, blocks)):
                for z in range(size_z):
                    mixed[1, pair, z, sample, some, :] = out[z * part_z : (z + 1) * part_z]
            return carry

        lax.fori_loop(0, size_z, body, 0)

    def along_y(pair):
        def body(block, carry):
            blocks = [
                [qkv[1, pair * 3 + m, block, sample] for m in range(3)] for sample in range(samples)
            ]
            for sample, out in enumerate(attend(1, pair, blocks)):
                for y in range(size_y):
                    ymixed[pair, y, block * samples + sample] = out[y * part_y : (y + 1) * part_y]
            return carry

        lax.fori_loop(0, size_z, body, 0)

    def add_up(pair):
        def body(block, carry):
            for sample in range(samples):
                there = jnp.concatenate(
                    [back[pair, y, block * samples + sample] for y in range(size_y)], axis=0
                )
                value = mixed[0, pair, block, sample].astype(jnp.float32) + there.astype(jnp.float32)
                value = value + mixed[1, pair, block, sample].astype(jnp.float32)
                summed[pair, block, sample] = value.astype(jnp.bfloat16)
            return carry

        for copy in returns(pair):
            copy.wait_recv()
        back[pair, me_y] = ymixed[pair, me_y]
        lax.fori_loop(0, size_z, body, 0)
        for copy in sums_out(pair):
            copy.start()
        parts[pair, me_z] = summed[pair, me_z]

    def output(pair):
        for copy in sums_out(pair):
            copy.wait_recv()
        left = jnp.concatenate(
            [parts[pair, z].reshape(samples * rows, wide) for z in range(size_z)], axis=1
        )
        for block in range(0, features // wide, 2):
            right = jnp.concatenate(
                [
                    jnp.concatenate(
                        [
                            wo[block + n, (z * pairs + pair) * wide : (z * pairs + pair + 1) * wide]
                            for z in range(size_z)
                        ],
                        axis=0,
                    )
                    for n in range(2)
                ],
                axis=1,
            )
            product = jnp.dot(left, right, preferred_element_type=jnp.float32)
            cols = slice(block * wide, (block + 2) * wide)
            if pair > 0:
                product = product + total[:, cols]
            if pair < pairs - 1:
                total[:, cols] = product
            else:
                residual = tokens[:, :, cols].astype(jnp.float32)
                result[:, :, cols] = (residual + product.reshape(residual.shape)).astype(jnp.bfloat16)

    early = 4
    for item in range(early):
        own_blocks(item)
    for sample in range(samples):
        spread_piece(sample)
    own_weights()
    lines[1, me_z, :, pl.ds(pl.multiple_of(me_y * part_y, part_y), part_y), :] = lines[
        0, me_z, :, pl.ds(pl.multiple_of(me_y * part_y, part_y), part_y), :
    ]
    bias_tables()
    chains(0, early)
    for step in range(1, size_y):
        exchange(step).start()
    spread_piece(samples)
    for item in range(early, items):
        own_blocks(item)
    pass_on(0)
    for item in range(2):
        from_side(item)
    for sample in range(samples):
        to_twin(sample, twin).wait_recv()
    project(0, 0, flank)
    for item in range(2, 4):
        from_side(item)
    project(0, 1, flank)
    pass_on(1)
    for step in range(1, 4):
        exchange_in(step)
    for sample in range(samples):
        relay(sample).wait_recv()
    project(0, 0, 1 - flank)
    project(0, 1, 1 - flank)
    along_x(0)
    for step in range(4, size_y):
        exchange_in(step)
    chains(early, items)
    along_z(0)
    for step in range(size_y):
        pass_on(samples + step)
    for step in range(size_y):
        to_twin(samples + step, twin).wait_recv()
    for item in range(slots, items):
        from_side(item)
    share_out(0, me_z, far).start()
    share_out(1, me_z, twin).start()
    project(1, 0, flank)
    project(1, 1, flank)
    for step in range(size_y):
        relay(samples + step).wait_recv()
    project(1, 0, 1 - flank)
    project(1, 1, 1 - flank)
    along_y(0)
    for copy in returns(0):
        copy.start()
    for item in range(early, slots):
        from_side(item)
    project(1, 2, flank)
    project(1, 2, 1 - flank)
    along_y(1)
    for copy in returns(1):
        copy.start()
    project(0, 2, flank)
    project(0, 2, 1 - flank)
    along_x(1)
    add_up(0)
    along_z(1)
    share_out(0, far, far).wait_recv()
    share_out(2, far, twin).start()
    add_up(1)
    share_out(1, twin, twin).wait_recv()
    share_out(2, 0, twin).wait_recv()
    output(0)
    output(1)
    for item in range(items):
        drain(item)
    for index in range(pieces):
        to_far(index).wait_send()
        to_twin(index).wait_send()
        relay(index).wait_send()
    for step in range(1, size_y):
        exchange(step).wait_send()
    for slot in range(3):
        share_out(slot, me_z, twin).wait_send()
    for pair in range(pairs):
        for copy in returns(pair) + sums_out(pair):
            copy.wait_send()


VMEM = pl.BlockSpec(memory_space=pltpu.VMEM)
DMA = pltpu.SemaphoreType.DMA


def fast_shards(size_y, size_z, tokens, w_qkv, w_out, bias_x, bias_y, bias_z):
    samples, depth, rows_y, rows_z, features = tokens.shape
    rows = depth * rows_y * rows_z
    levels = size_y // 2
    wide = 2 * HEAD
    pairs = HEADS // (2 * size_z)
    items = 4 * pairs
    pieces = samples + size_y
    lengths = [(table.shape[1] + 1) // 2 for table in (bias_x, bias_y, bias_z)]
    width = -(-max(2 * length - 1 for length in lengths) // 128) * 128
    lookup = offset_lookup(line_places(rows, size_y, size_z, rows_z), lengths, rows, width)
    block = (samples, rows, features)
    piled = (pairs, size_z, samples, rows, wide)
    sliced = (pairs, size_y, size_z * samples, rows // size_y, wide)
    result = pl.pallas_call(
        functools.partial(heads_kernel, size_y, size_z, rows_z),
        out_shape=jax.ShapeDtypeStruct(block, jnp.bfloat16),
        in_specs=[VMEM] * 7,
        out_specs=VMEM,
        scratch_shapes=[
            pltpu.VMEM((2, size_z) + block, jnp.bfloat16),
            pltpu.VMEM((3 * pairs, features, wide), jnp.bfloat16),
            pltpu.VMEM((features // wide, features, wide), jnp.bfloat16),
            pltpu.VMEM((3, HEADS, width), jnp.float32),
            pltpu.VMEM((3, HEADS, 2 * rows), jnp.float32),
            pltpu.VMEM((3, 2 * pairs, rows, rows), jnp.float32),
            pltpu.VMEM((2, 3 * pairs, size_z, samples, rows, wide), jnp.bfloat16),
            pltpu.VMEM((2,) + piled, jnp.bfloat16),
            pltpu.VMEM(sliced, jnp.bfloat16),
            pltpu.VMEM(sliced, jnp.bfloat16),
            pltpu.VMEM(piled, jnp.bfloat16),
            pltpu.VMEM(piled, jnp.bfloat16),
            pltpu.VMEM((samples * rows, features), jnp.float32),
        ]
        + [DMA((items, levels))] * 6
        + [DMA((size_y - 1,))] * 2
        + [DMA((pieces,))] * 6
        + [DMA((3,))] * 2
        + [DMA((pairs, size_y - 1))] * 2
        + [DMA((pairs, size_z - 1))] * 2,
        compiler_params=pltpu.CompilerParams(collective_id=0, has_side_effects=True),
    )(tokens.reshape(block), w_qkv, w_out, bias_x, bias_y, bias_z, jnp.asarray(lookup))
    return result.reshape(tokens.shape)


def body_for(size_y, size_z):
    def body(tokens, *parameters):
        _, depth, rows_y, rows_z, features = tokens.shape
        rows = depth * rows_y * rows_z
        fits = size_y % 2 == 0 and size_z == 4 and HEADS % (4 * size_z) == 0 and rows == 2 * HEAD
        if fits and rows_y == 1 and rows % (16 * size_y) == 0 and rows % (16 * size_z) == 0:
            return fast_shards(size_y, size_z, tokens, *parameters)
        return shards(tokens, *parameters)

    return body


def solution(mesh):
    placed = (P(None, None, "gy", "gz", None), P("gy", None), P("gy", None), P(), P(), P())
    return jax.shard_map(
        body_for(mesh.shape["gy"], mesh.shape["gz"]),
        mesh=mesh,
        in_specs=placed,
        out_specs=P(None, None, "gy", "gz", None),
        check_vma=False,
    )
```

```python
import functools

import jax
import jax.numpy as jnp
import numpy as np
from jax import lax
from jax.experimental import pallas as pl
from jax.experimental.pallas import tpu as pltpu
from jax.sharding import PartitionSpec as P

HEADS = 16
HEAD = 64


einsum_forms = {
    1: ("bxyzhs,bwyzhs->byzhxw", "byzhxw,bwyzhs->bxyzhs"),
    2: ("bxyzhs,bxwzhs->bxzhyw", "bxzhyw,bxwzhs->bxyzhs"),
    3: ("bxyzhs,bxywhs->bxyhzw", "bxyhzw,bxywhs->bxyzhs"),
}


def norm_rows(tokens):
    values = tokens.astype(jnp.float32)
    center = jnp.mean(values, axis=-1, keepdims=True)
    spread = jnp.mean((values - center) ** 2, axis=-1, keepdims=True)
    return ((values - center) * lax.rsqrt(spread + 1e-05)).astype(jnp.bfloat16)


def rel_bias(table):
    length = (table.shape[1] + 1) // 2
    offsets = (
        lax.broadcasted_iota(jnp.int32, (length, length), 0)
        - lax.broadcasted_iota(jnp.int32, (length, length), 1)
        + length
        - 1
    )
    lookup = (
        offsets[:, :, None] == lax.broadcasted_iota(jnp.int32, (1, 1, 2 * length - 1), 2)
    ).astype(jnp.float32)
    return jnp.einsum("hr,ijr->hij", table, lookup, precision=lax.Precision.HIGHEST)


def attend(qkv, table, axis):
    dims = qkv.shape
    features = dims[-1] // 3
    parts = qkv.reshape(dims[:-1] + (3, HEADS, HEAD))
    query = parts[..., 0, :, :]
    keys = parts[..., 1, :, :]
    values = parts[..., 2, :, :]
    score_form, mix_form = einsum_forms[axis]
    scores = jnp.einsum(score_form, query, keys, preferred_element_type=jnp.float32) * HEAD ** (
        -0.5
    ) + rel_bias(table)
    scores = scores - jnp.max(scores, axis=-1, keepdims=True)
    expo = jnp.exp(scores)
    weights = (expo / jnp.sum(expo, axis=-1, keepdims=True)).astype(jnp.bfloat16)
    mixed = jnp.einsum(mix_form, weights, values, preferred_element_type=jnp.float32)
    return mixed.reshape(dims[:-1] + (features,)).astype(jnp.bfloat16)


def return_y(result):
    return lax.all_to_all(result, "gy", split_axis=2, concat_axis=1, tiled=True)


def return_z(result):
    return lax.all_to_all(result, "gz", split_axis=3, concat_axis=1, tiled=True)


def shards(tokens, w_qkv, w_out, bias_x, bias_y, bias_z):
    samples, depth, rows_y, rows_z, features = tokens.shape
    normed = norm_rows(tokens)
    gathered = lax.all_gather(w_qkv, "gy", axis=0, tiled=True)

    def project(inputs):
        product = jnp.dot(
            inputs.reshape(-1, features), gathered, preferred_element_type=jnp.float32
        )
        return product.astype(jnp.bfloat16).reshape(inputs.shape[:-1] + (3 * features,))

    along_x = attend(project(normed), bias_x, 1)
    along_y = return_y(
        attend(
            project(lax.all_to_all(normed, "gy", split_axis=1, concat_axis=2, tiled=True)),
            bias_y,
            2,
        )
    )
    along_z = return_z(
        attend(
            project(lax.all_to_all(normed, "gz", split_axis=1, concat_axis=3, tiled=True)),
            bias_z,
            3,
        )
    )
    summed = along_x.astype(jnp.float32) + along_y.astype(jnp.float32) + along_z.astype(jnp.float32)
    summed = summed.astype(jnp.bfloat16).reshape(-1, features)
    residual = tokens.reshape(-1, features).astype(jnp.float32)
    result = residual + jnp.dot(
        summed, lax.all_gather(w_out, "gy", axis=0, tiled=True), preferred_element_type=jnp.float32
    )
    return result.astype(jnp.bfloat16).reshape(tokens.shape)


def device(**where):
    return {"device_id": where, "device_id_type": pl.DeviceIdType.MESH}


def line_places(rows, size_y, size_z, rows_z):
    row = np.arange(rows)
    part_y, part_z = rows // size_y, rows // size_z
    return (
        (row // rows_z, row % rows_z),
        (row // part_y, row % part_y),
        (row // part_z * rows_z + row % rows_z, row % part_z // rows_z),
    )


def offset_lookup(places, lengths, rows, width):
    lookup = np.zeros((len(lengths), width, 2 * rows), np.float32)
    for axis, ((position, line), length) in enumerate(zip(places, lengths)):
        first, second = np.nonzero(line[:, None] == line[None, :])
        entry = position[first] - position[second] + length - 1
        lookup[axis, entry, rows - 1 - first + second] = 1.0
    return lookup


def remote(source, target, sends, recvs, **where):
    return pltpu.make_async_remote_copy(
        src_ref=source, dst_ref=target, send_sem=sends, recv_sem=recvs, **device(**where)
    )


def heads_kernel(
    size_y, size_z, tokens_in, w_qkv, w_out, bias_x_in, bias_y_in, bias_z_in, lookup_in, result,
    tokens, bias_x, bias_y, bias_z, lookup, in_sem, own_sem, lines, wq, wo, padded, offsets, biases, qkv, mixed, ymixed, back, summed, parts, total,
    up_send, up_recv, down_send, down_recv, side_send, side_recv,
    y_send, y_recv, far_send, far_recv, twin_send, twin_recv, relay_send, relay_recv,
    o_send, o_recv, of_send, of_recv, ry_send, ry_recv, ez_send, ez_recv,
):
    me_y, me_z = lax.axis_index("gy"), lax.axis_index("gz")
    samples, length, rows_z, features = tokens.shape
    rows = length * rows_z
    depth = w_qkv.shape[0]
    wide = 2 * HEAD
    pairs = HEADS // (2 * size_z)
    slots = 3 * pairs
    items = slots + pairs
    levels = size_y // 2
    part_y, part_z = rows // size_y, rows // size_z
    level, side = me_y // 2, lax.rem(me_y, 2)
    core, flank = lax.rem(me_z, 2), me_z // 2
    above, below = {"gy": me_y + 2}, {"gy": me_y - 2}
    beside = {"gy": level * 2 + 1 - side}
    twin = me_z + 1 - 2 * core
    far = me_z + 2 - 4 * flank

    inputs = [
        pltpu.make_async_copy(source, target, in_sem.at[index])
        for index, (source, target) in enumerate(
            (
                (tokens_in, tokens), (bias_x_in, bias_x), (bias_y_in, bias_y),
                (bias_z_in, bias_z), (lookup_in, lookup),
            )
        )
    ]
    for copy in inputs:
        copy.start()

    barrier = pltpu.get_barrier_semaphore()
    for dist in (1, 2):
        pl.when(level + dist < levels)(
            lambda: pl.semaphore_signal(barrier, inc=1, **device(gy=me_y + 2 * dist))
        )
        pl.when(level - dist >= 0)(
            lambda: pl.semaphore_signal(barrier, inc=1, **device(gy=me_y - 2 * dist))
        )
    pl.semaphore_signal(barrier, inc=1, **device(**beside))
    pl.semaphore_signal(barrier, inc=1, **device(gz=twin))
    pl.semaphore_signal(barrier, inc=1, **device(gz=far))
    near = jnp.minimum(level, 2) + jnp.minimum(levels - 1 - level, 2)
    pl.semaphore_wait(barrier, near + 3)

    def item_ref(item):
        return wq.at[item] if item < slots else wo.at[me_z * pairs + item - slots]

    def own_ref(item):
        if item < slots:
            start = item % 3 * features + (me_z * pairs + item // 3) * wide
            return w_qkv.at[:, pl.ds(pl.multiple_of(start, wide), wide)]
        start = (me_z * pairs + item - slots) * wide
        return w_out.at[:, pl.ds(pl.multiple_of(start, wide), wide)]

    def transfer(item, lev, sid, sends, recvs, slot, where, own=False):
        block = item_ref(item).at[pl.ds(pl.multiple_of((lev * 2 + sid) * depth, depth), depth)]
        source = own_ref(item) if own else block
        return remote(source, block, sends.at[item, slot], recvs.at[item, slot], **where)

    def up(item, step, own=False):
        return transfer(item, level - step, side, up_send, up_recv, step, above, own)

    def up_in(item, step):
        return transfer(item, level - 1 - step, side, up_send, up_recv, step, above)

    def down(item, step, own=False):
        return transfer(item, level + step, side, down_send, down_recv, step, below, own)

    def down_in(item, step):
        return transfer(item, level + 1 + step, side, down_send, down_recv, step, below)

    def across(item, lev, own=False):
        return transfer(item, lev, side, side_send, side_recv, lev, beside, own)

    def across_in(item, lev):
        return transfer(item, lev, 1 - side, side_send, side_recv, lev, beside)

    def far_block(item, lev, sid, gz, own=False):
        part, index = item - slots, lev * 2 + sid
        ref = wo.at[gz * pairs + part].at[pl.ds(pl.multiple_of(index * depth, depth), depth)]
        source = own_ref(item) if own else ref
        return remote(source, ref, of_send.at[part, index], of_recv.at[part, index], gz=far)

    def block_out(item, lev, sid, own=False):
        if item >= slots:
            far_block(item, lev, sid, me_z, own).start()

    def own_blocks(item):
        pl.when(level + 1 < levels)(lambda: up(item, 0, True).start())
        pl.when(level > 0)(lambda: down(item, 0, True).start())
        across(item, level, True).start()
        block_out(item, level, side, True)

    def chain(item, step):
        @pl.when(level - 1 - step >= 0)
        def _():
            up_in(item, step).wait_recv()
            pl.when(level + 1 < levels)(lambda: up(item, step + 1).start())
            across(item, level - 1 - step).start()
            block_out(item, level - 1 - step, side)

        @pl.when(level + 1 + step < levels)
        def _():
            down_in(item, step).wait_recv()
            pl.when(level > 0)(lambda: down(item, step + 1).start())
            across(item, level + 1 + step).start()
            block_out(item, level + 1 + step, side)

    def reach(item, dist, rise, passed=False):
        sends, recvs = (up_send, up_recv) if rise else (down_send, down_recv)
        sign = 1 if rise else -1
        if passed:
            return transfer(item, level - 2 * sign, side, sends, recvs, 2, {"gy": me_y + 2 * sign})
        return transfer(
            item, level, side, sends, recvs, dist - 1, {"gy": me_y + 2 * sign * dist}, True
        )

    def direct(item):
        across(item, level, True).start()
        for dist in (1, 2):
            pl.when(level + dist < levels)(lambda: reach(item, dist, True).start())
            pl.when(level - dist >= 0)(lambda: reach(item, dist, False).start())
        block_out(item, level, side, True)

    def arrive(item, dist):
        @pl.when(level - dist >= 0)
        def _():
            reach(item, dist, True, dist == 3).wait_recv()
            if dist == 2:
                pl.when(level + 1 < levels)(lambda: reach(item, 3, True, True).start())
            across(item, level - dist).start()
            block_out(item, level - dist, side)

        @pl.when(level + dist < levels)
        def _():
            reach(item, dist, False, dist == 3).wait_recv()
            if dist == 2:
                pl.when(level > 0)(lambda: reach(item, 3, False, True).start())
            across(item, level + dist).start()
            block_out(item, level + dist, side)

    def drain_direct(item):
        across(item, level, True).wait_send()
        for dist in range(1, levels):

            @pl.when(level + dist < levels)
            def _():
                if dist < 3:
                    reach(item, dist, True).wait_send()
                across(item, level + dist).wait_send()

            @pl.when(level - dist >= 0)
            def _():
                if dist < 3:
                    reach(item, dist, False).wait_send()
                across(item, level - dist).wait_send()

        pl.when(jnp.logical_and(level >= 2, level + 1 < levels))(
            lambda: reach(item, 3, True, True).wait_send()
        )
        pl.when(jnp.logical_and(level + 2 < levels, level > 0))(
            lambda: reach(item, 3, False, True).wait_send()
        )

    def from_side(item):
        for lev in range(levels):
            across_in(item, lev).wait_recv()
            block_out(item, lev, 1 - side)

    def drain(item):
        pl.when(level + 1 < levels)(lambda: up(item, 0, True).wait_send())
        pl.when(level > 0)(lambda: down(item, 0, True).wait_send())
        across(item, level, True).wait_send()
        for step in range(1, levels):

            @pl.when(level - step >= 0)
            def _():
                pl.when(level + 1 < levels)(lambda: up(item, step).wait_send())
                across(item, level - step).wait_send()

            @pl.when(level + step < levels)
            def _():
                pl.when(level > 0)(lambda: down(item, step).wait_send())
                across(item, level + step).wait_send()

    pieces = samples + size_y

    def piece_of(index, block):
        if index < samples:
            return lines.at[0, block, index]
        peer = lax.rem(me_y + size_y - (index - samples), size_y)
        return lines.at[1, block, :, pl.ds(pl.multiple_of(peer * part_y, part_y), part_y), :]

    def to_far(index, block=me_z):
        ref = piece_of(index, block)
        return remote(ref, ref, far_send.at[index], far_recv.at[index], gz=far)

    def to_twin(index, block=me_z):
        ref = piece_of(index, block)
        return remote(ref, ref, twin_send.at[index], twin_recv.at[index], gz=twin)

    def relay(index, block=far):
        ref = piece_of(index, block)
        return remote(ref, ref, relay_send.at[index], relay_recv.at[index], gz=twin)

    def spread_piece(index):
        to_far(index).start()
        to_twin(index).start()

    def pass_on(index):
        to_far(index, far).wait_recv()
        relay(index).start()

    def exchange(step):
        peer = lax.rem(me_y + step, size_y)
        return remote(
            lines.at[0, me_z, :, pl.ds(pl.multiple_of(peer * part_y, part_y), part_y), :],
            lines.at[1, me_z, :, pl.ds(pl.multiple_of(me_y * part_y, part_y), part_y), :],
            y_send.at[step - 1], y_recv.at[step - 1], gy=peer,
        )

    def exchange_in(step):
        exchange(step).wait_recv()
        spread_piece(samples + step)

    def share_out(slot, part, block):
        ref = wo.at[block * pairs + part]
        return remote(ref, ref, o_send.at[slot, part], o_recv.at[slot, part], gz=twin)

    def share(part):
        from_side(slots + part)
        share_out(0, part, me_z).start()

    def relay_share(part):
        for index in range(size_y):
            far_block(slots + part, 0, index, far).wait_recv()
        share_out(1, part, far).start()

    def shared(part):
        share_out(0, part, twin).wait_recv()
        share_out(1, part, far).wait_recv()

    def returns(pair, where):
        some = pl.ds(pl.multiple_of(where * 2 * samples, 2 * samples), 2 * samples)
        there = jnp.where(where == flank, 0, 1)
        copies = []
        for step in range(1, size_y):
            peer = lax.rem(me_y + step, size_y)
            copies.append(
                remote(
                    ymixed.at[pair, peer, some], back.at[pair, me_y, some],
                    ry_send.at[pair, there, step - 1], ry_recv.at[pair, there, step - 1], gy=peer,
                )
            )
        return copies

    def give_back(pair, where):
        along_y(pair, where)
        for copy in returns(pair, where):
            copy.start()

    def sum_out(pair, peer, slot):
        return remote(
            summed.at[pair, peer], parts.at[pair, me_z],
            ez_send.at[pair, slot], ez_recv.at[pair, slot], gz=peer,
        )

    def sums_out(pair, where):
        if where is flank:
            return [sum_out(pair, twin, 0)]
        return [sum_out(pair, far, 1), sum_out(pair, far + twin - me_z, 2)]

    row = lax.broadcasted_iota(jnp.int32, (rows, rows), 0)
    col = lax.broadcasted_iota(jnp.int32, (rows, rows), 1)
    lane = lax.broadcasted_iota(jnp.int32, (rows, wide), 1)
    line_of = (
        lambda r: lax.rem(r, rows_z),
        lambda r: lax.rem(r, part_y),
        lambda r: lax.rem(r, part_z) // rows_z,
    )

    def own_copy(item):
        mine = pl.ds(pl.multiple_of(me_y * depth, depth), depth)
        return pltpu.make_async_copy(own_ref(item), item_ref(item).at[mine], own_sem.at[item])

    def normalize():
        inputs[0].wait()
        values = tokens[...].astype(jnp.float32).reshape(samples, rows, features)
        center = jnp.mean(values, axis=-1, keepdims=True)
        spread = jnp.mean((values - center) ** 2, axis=-1, keepdims=True)
        lines[0, me_z] = ((values - center) * lax.rsqrt(spread + 1e-05)).astype(jnp.bfloat16)

    def bias_tables():
        for copy in inputs[1:]:
            copy.wait()
        padded[...] = jnp.zeros(padded.shape, jnp.float32)
        for axis, table in enumerate((bias_x, bias_y, bias_z)):
            padded[axis, :, : table.shape[1]] = table[...]
            offsets[axis] = jnp.dot(
                padded[axis], lookup[axis],
                precision=lax.Precision.HIGHEST, preferred_element_type=jnp.float32,
            )

        def fill(head, carry):
            for axis in range(3):
                same = line_of[axis](row) == line_of[axis](col)
                entry = offsets[axis, pl.ds(me_z * 2 * pairs + head, 1), :]
                table = jnp.broadcast_to(entry, (rows, 2 * rows))
                table = pltpu.roll(table, rows + 1, 1, stride=1, stride_axis=0)
                biases[axis, head] = jnp.where(same, table[:, :rows], -1e30)
            return carry

        lax.fori_loop(0, 2 * pairs, fill, 0)

    def project(group, chosen, where):
        blocks = pl.ds(pl.multiple_of(where * 2, 2), 2)
        flat = lines[group, blocks].reshape(2 * samples * rows, features)
        right = jnp.concatenate([wq[item] for item in chosen], axis=1)
        product = jnp.dot(flat, right, preferred_element_type=jnp.float32)
        for place, item in enumerate(chosen):
            piece = product[:, place * wide : (place + 1) * wide]
            if item % 3 == 0:
                piece = piece * HEAD ** (-0.5)
            qkv[group, item, blocks] = piece.astype(jnp.bfloat16).reshape(2, samples, rows, wide)

    def attend(axis, pair, blocks):
        units = [(block, odd) for block in range(len(blocks)) for odd in range(2)]
        scores, expos, totals, outs = {}, {}, {}, {}
        for unit in units:
            block, odd = unit
            query, keys, _ = blocks[block]
            chosen = jnp.where(lane // HEAD == odd, query, 0)
            scores[unit] = lax.dot_general(
                chosen, keys, (((1,), (1,)), ((), ())), preferred_element_type=jnp.float32
            ) + biases[axis, pair * 2 + odd]
        for unit in units:
            expos[unit] = jnp.exp(scores[unit] - jnp.max(scores[unit], axis=-1, keepdims=True))
            totals[unit] = jnp.sum(expos[unit], axis=-1, keepdims=True)
        for unit in units:
            outs[unit] = jnp.dot(
                expos[unit].astype(jnp.bfloat16), blocks[unit[0]][2],
                preferred_element_type=jnp.float32,
            )
        return [
            jnp.where(
                lane < HEAD,
                outs[block, 0] * (1.0 / totals[block, 0]),
                outs[block, 1] * (1.0 / totals[block, 1]),
            ).astype(jnp.bfloat16)
            for block in range(len(blocks))
        ]

    def along_x(pair, where):
        def body(block, carry):
            blocks = [
                [qkv[0, pair * 3 + m, block, sample] for m in range(3)] for sample in range(samples)
            ]
            for sample, out in enumerate(attend(0, pair, blocks)):
                mixed[0, pair, block, sample] = out
            return carry

        lax.fori_loop(where * 2, where * 2 + 2, body, 0)

    def along_z(pair):
        def body(index, carry):
            some = pl.ds(pl.multiple_of(index * part_z, part_z), part_z)
            blocks = [
                [
                    jnp.concatenate(
                        [qkv[0, pair * 3 + m, z, sample, some, :] for z in range(size_z)], axis=0
                    )
                    for m in range(3)
                ]
                for sample in range(samples)
            ]
            for sample, out in enumerate(attend(2, pair, blocks)):
                for z in range(size_z):
                    mixed[1, pair, z, sample, some, :] = out[z * part_z : (z + 1) * part_z]
            return carry

        lax.fori_loop(0, size_z, body, 0)

    def along_y(pair, where):
        def body(block, carry):
            blocks = [
                [qkv[1, pair * 3 + m, block, sample] for m in range(3)] for sample in range(samples)
            ]
            for sample, out in enumerate(attend(1, pair, blocks)):
                for y in range(size_y):
                    ymixed[pair, y, block * samples + sample] = out[y * part_y : (y + 1) * part_y]
            return carry

        lax.fori_loop(where * 2, where * 2 + 2, body, 0)

    def add_up(pair, where):
        def body(block, carry):
            for sample in range(samples):
                there = jnp.concatenate(
                    [back[pair, y, block * samples + sample] for y in range(size_y)], axis=0
                )
                value = mixed[0, pair, block, sample].astype(jnp.float32) + there.astype(jnp.float32)
                value = value + mixed[1, pair, block, sample].astype(jnp.float32)
                summed[pair, block, sample] = value.astype(jnp.bfloat16)
            return carry

        for copy in returns(pair, where):
            copy.wait_recv()
        some = pl.ds(pl.multiple_of(where * 2 * samples, 2 * samples), 2 * samples)
        back[pair, me_y, some] = ymixed[pair, me_y, some]
        lax.fori_loop(where * 2, where * 2 + 2, body, 0)
        for copy in sums_out(pair, where):
            copy.start()
        if where is flank:
            parts[pair, me_z] = summed[pair, me_z]

    def output(pair):
        for where in (1 - flank, flank):
            for copy in sums_out(pair, where):
                copy.wait_recv()
        left = jnp.concatenate(
            [parts[pair, z].reshape(samples * rows, wide) for z in range(size_z)], axis=1
        )
        for block in range(0, features // wide, 2):
            right = jnp.concatenate(
                [
                    jnp.concatenate(
                        [
                            wo[block + n, (z * pairs + pair) * wide : (z * pairs + pair + 1) * wide]
                            for z in range(size_z)
                        ],
                        axis=0,
                    )
                    for n in range(2)
                ],
                axis=1,
            )
            product = jnp.dot(left, right, preferred_element_type=jnp.float32)
            cols = slice(block * wide, (block + 2) * wide)
            if pair > 0:
                product = product + total[:, cols]
            if pair < pairs - 1:
                total[:, cols] = product
            else:
                residual = tokens[:, :, :, cols].astype(jnp.float32).reshape(samples, rows, 2 * wide)
                result[:, :, cols] = (residual + product.reshape(residual.shape)).astype(jnp.bfloat16)

    other = 1 - flank
    straight = (0, 1, 2)
    own_rows = pl.ds(pl.multiple_of(me_y * part_y, part_y), part_y)
    hops = levels - 1
    order = [4, 2, 6, 3, 5, 1, 7]

    def waves(first, last):
        return [
            [(wave - step, step) for step in range(hops) if first <= wave - step < last]
            for wave in range(first, last + hops - 1)
        ]

    def run(wave):
        for item, step in wave:
            chain(item, step)

    for item in straight:
        direct(item)
    for item in range(items):
        own_copy(item).start()
    normalize()
    for sample in range(samples):
        spread_piece(sample)
    lines[1, me_z, :, own_rows, :] = lines[0, me_z, :, own_rows, :]
    for dist in (1, 2):
        for item in straight:
            arrive(item, dist)
    bias_tables()
    for item in straight:
        arrive(item, 3)
    for step in order[:3]:
        exchange(step).start()
    from_side(0)
    for step in order[3:]:
        exchange(step).start()
    spread_piece(samples)
    for item in range(3, 6):
        own_blocks(item)
    for item in range(items):
        own_copy(item).wait()
    pass_on(0)
    for item in range(1, 3):
        from_side(item)
    for sample in range(samples):
        to_twin(sample, twin).wait_recv()
    project(0, (0, 1, 2), flank)
    exchange_in(order[0])
    pass_on(1)
    along_x(0, flank)
    exchange_in(order[1])
    exchange_in(order[2])
    for sample in range(samples):
        relay(sample).wait_recv()
    project(0, (0, 1, 2), other)
    exchange_in(order[3])
    for item in range(6, 8):
        own_blocks(item)
    wave = waves(3, 8)
    run(wave[0])
    along_x(0, other)
    exchange_in(order[4])
    exchange_in(order[5])
    run(wave[1])
    along_z(0)
    exchange_in(order[6])
    run(wave[2])
    pass_on(samples)
    for step in order[:2]:
        pass_on(samples + step)
    for step in range(size_y):
        to_twin(samples + step, twin).wait_recv()
    project(1, (0, 1, 2), flank)
    run(wave[3])
    give_back(0, flank)
    run(wave[4])
    for step in order[2:]:
        pass_on(samples + step)
    for step in range(size_y):
        relay(samples + step).wait_recv()
    project(1, (0, 1, 2), other)
    give_back(0, other)
    run(wave[5])
    for item in range(3, 6):
        from_side(item)
    project(1, (3, 4, 5), other)
    give_back(1, other)
    run(wave[6])
    project(1, (3, 4, 5), flank)
    give_back(1, flank)
    share(0)
    project(0, (3, 4, 5), other)
    share(1)
    project(0, (3, 4, 5), flank)
    add_up(0, other)
    add_up(0, flank)
    along_x(1, other)
    along_z(1)
    add_up(1, other)
    along_x(1, flank)
    add_up(1, flank)
    relay_share(0)
    relay_share(1)
    shared(0)
    shared(1)
    output(0)
    output(1)
    for item in range(items):
        if item in straight:
            drain_direct(item)
        else:
            drain(item)
    for index in range(pieces):
        to_far(index).wait_send()
        to_twin(index).wait_send()
        relay(index).wait_send()
    for step in range(1, size_y):
        exchange(step).wait_send()
    for part in range(pairs):
        for slot in range(2):
            share_out(slot, part, me_z).wait_send()
        for index in range(size_y):
            far_block(slots + part, 0, index, me_z).wait_send()
    for pair in range(pairs):
        for where in (other, flank):
            for copy in returns(pair, where) + sums_out(pair, where):
                copy.wait_send()


VMEM = pl.BlockSpec(memory_space=pltpu.VMEM)
DMA = pltpu.SemaphoreType.DMA


def fast_shards(size_y, size_z, tokens, w_qkv, w_out, bias_x, bias_y, bias_z):
    samples, depth, rows_y, rows_z, features = tokens.shape
    rows = depth * rows_y * rows_z
    levels = size_y // 2
    wide = 2 * HEAD
    pairs = HEADS // (2 * size_z)
    items = 4 * pairs
    pieces = samples + size_y
    lengths = [(table.shape[1] + 1) // 2 for table in (bias_x, bias_y, bias_z)]
    width = -(-max(2 * length - 1 for length in lengths) // 128) * 128
    lookup = offset_lookup(line_places(rows, size_y, size_z, rows_z), lengths, rows, width)
    given = (samples, depth, rows_z, features)
    block = (samples, rows, features)
    piled = (pairs, size_z, samples, rows, wide)
    sliced = (pairs, size_y, size_z * samples, rows // size_y, wide)
    result = pl.pallas_call(
        functools.partial(heads_kernel, size_y, size_z),
        out_shape=jax.ShapeDtypeStruct(block, jnp.bfloat16),
        in_specs=[pl.BlockSpec(memory_space=pl.ANY)] * 7,
        out_specs=VMEM,
        scratch_shapes=[
            pltpu.VMEM(given, jnp.bfloat16),
            pltpu.VMEM(bias_x.shape, jnp.float32),
            pltpu.VMEM(bias_y.shape, jnp.float32),
            pltpu.VMEM(bias_z.shape, jnp.float32),
            pltpu.VMEM(lookup.shape, jnp.float32),
            DMA((5,)), DMA((items,)),
            pltpu.VMEM((2, size_z) + block, jnp.bfloat16),
            pltpu.VMEM((3 * pairs, features, wide), jnp.bfloat16),
            pltpu.VMEM((features // wide, features, wide), jnp.bfloat16),
            pltpu.VMEM((3, HEADS, width), jnp.float32),
            pltpu.VMEM((3, HEADS, 2 * rows), jnp.float32),
            pltpu.VMEM((3, 2 * pairs, rows, rows), jnp.float32),
            pltpu.VMEM((2, 3 * pairs, size_z, samples, rows, wide), jnp.bfloat16),
            pltpu.VMEM((2,) + piled, jnp.bfloat16),
            pltpu.VMEM(sliced, jnp.bfloat16),
            pltpu.VMEM(sliced, jnp.bfloat16),
            pltpu.VMEM(piled, jnp.bfloat16),
            pltpu.VMEM(piled, jnp.bfloat16),
            pltpu.VMEM((samples * rows, features), jnp.float32),
        ]
        + [DMA((items, levels))] * 6
        + [DMA((size_y - 1,))] * 2
        + [DMA((pieces,))] * 6
        + [DMA((2, pairs))] * 2
        + [DMA((pairs, size_y))] * 2
        + [DMA((pairs, 2, size_y - 1))] * 2
        + [DMA((pairs, size_z - 1))] * 2,
        compiler_params=pltpu.CompilerParams(collective_id=0, has_side_effects=True),
    )(tokens.reshape(given), w_qkv, w_out, bias_x, bias_y, bias_z, jnp.asarray(lookup))
    return result.reshape(tokens.shape)


def body_for(size_y, size_z):
    def body(tokens, *parameters):
        _, depth, rows_y, rows_z, features = tokens.shape
        rows = depth * rows_y * rows_z
        fits = size_y == 8 and size_z == 4 and HEADS % (4 * size_z) == 0 and rows == 2 * HEAD
        if fits and rows_y == 1 and rows % (16 * size_y) == 0 and rows % (16 * size_z) == 0:
            return fast_shards(size_y, size_z, tokens, *parameters)
        return shards(tokens, *parameters)

    return body


def solution(mesh):
    placed = (P(None, None, "gy", "gz", None), P("gy", None), P("gy", None), P(), P(), P())
    return jax.shard_map(
        body_for(mesh.shape["gy"], mesh.shape["gz"]),
        mesh=mesh,
        in_specs=placed,
        out_specs=P(None, None, "gy", "gz", None),
        check_vma=False,
    )
```

```python
import functools

import jax
import jax.numpy as jnp
import numpy as np
from jax import lax
from jax.experimental import pallas as pl
from jax.experimental.pallas import tpu as pltpu
from jax.sharding import PartitionSpec as P

HEADS = 16
HEAD = 64


einsum_forms = {
    1: ("bxyzhs,bwyzhs->byzhxw", "byzhxw,bwyzhs->bxyzhs"),
    2: ("bxyzhs,bxwzhs->bxzhyw", "bxzhyw,bxwzhs->bxyzhs"),
    3: ("bxyzhs,bxywhs->bxyhzw", "bxyhzw,bxywhs->bxyzhs"),
}


def norm_rows(tokens):
    values = tokens.astype(jnp.float32)
    center = jnp.mean(values, axis=-1, keepdims=True)
    spread = jnp.mean((values - center) ** 2, axis=-1, keepdims=True)
    return ((values - center) * lax.rsqrt(spread + 1e-05)).astype(jnp.bfloat16)


def rel_bias(table):
    length = (table.shape[1] + 1) // 2
    offsets = (
        lax.broadcasted_iota(jnp.int32, (length, length), 0)
        - lax.broadcasted_iota(jnp.int32, (length, length), 1)
        + length
        - 1
    )
    lookup = (
        offsets[:, :, None] == lax.broadcasted_iota(jnp.int32, (1, 1, 2 * length - 1), 2)
    ).astype(jnp.float32)
    return jnp.einsum("hr,ijr->hij", table, lookup, precision=lax.Precision.HIGHEST)


def attend(qkv, table, axis):
    dims = qkv.shape
    features = dims[-1] // 3
    parts = qkv.reshape(dims[:-1] + (3, HEADS, HEAD))
    query = parts[..., 0, :, :]
    keys = parts[..., 1, :, :]
    values = parts[..., 2, :, :]
    score_form, mix_form = einsum_forms[axis]
    scores = jnp.einsum(score_form, query, keys, preferred_element_type=jnp.float32) * HEAD ** (
        -0.5
    ) + rel_bias(table)
    scores = scores - jnp.max(scores, axis=-1, keepdims=True)
    expo = jnp.exp(scores)
    weights = (expo / jnp.sum(expo, axis=-1, keepdims=True)).astype(jnp.bfloat16)
    mixed = jnp.einsum(mix_form, weights, values, preferred_element_type=jnp.float32)
    return mixed.reshape(dims[:-1] + (features,)).astype(jnp.bfloat16)


def return_y(result):
    return lax.all_to_all(result, "gy", split_axis=2, concat_axis=1, tiled=True)


def return_z(result):
    return lax.all_to_all(result, "gz", split_axis=3, concat_axis=1, tiled=True)


def shards(tokens, w_qkv, w_out, bias_x, bias_y, bias_z):
    samples, depth, rows_y, rows_z, features = tokens.shape
    normed = norm_rows(tokens)
    gathered = lax.all_gather(w_qkv, "gy", axis=0, tiled=True)

    def project(inputs):
        product = jnp.dot(
            inputs.reshape(-1, features), gathered, preferred_element_type=jnp.float32
        )
        return product.astype(jnp.bfloat16).reshape(inputs.shape[:-1] + (3 * features,))

    along_x = attend(project(normed), bias_x, 1)
    along_y = return_y(
        attend(
            project(lax.all_to_all(normed, "gy", split_axis=1, concat_axis=2, tiled=True)),
            bias_y,
            2,
        )
    )
    along_z = return_z(
        attend(
            project(lax.all_to_all(normed, "gz", split_axis=1, concat_axis=3, tiled=True)),
            bias_z,
            3,
        )
    )
    summed = along_x.astype(jnp.float32) + along_y.astype(jnp.float32) + along_z.astype(jnp.float32)
    summed = summed.astype(jnp.bfloat16).reshape(-1, features)
    residual = tokens.reshape(-1, features).astype(jnp.float32)
    result = residual + jnp.dot(
        summed, lax.all_gather(w_out, "gy", axis=0, tiled=True), preferred_element_type=jnp.float32
    )
    return result.astype(jnp.bfloat16).reshape(tokens.shape)


def device(**where):
    return {"device_id": where, "device_id_type": pl.DeviceIdType.MESH}


def line_places(rows, size_y, size_z, rows_z):
    row = np.arange(rows)
    part_y, part_z = rows // size_y, rows // size_z
    return (
        (row // rows_z, row % rows_z),
        (row // part_y, row % part_y),
        (row // part_z * rows_z + row % rows_z, row % part_z // rows_z),
    )


def offset_lookup(places, lengths, rows, width):
    lookup = np.zeros((len(lengths), width, 2 * rows), np.float32)
    for axis, ((position, line), length) in enumerate(zip(places, lengths)):
        first, second = np.nonzero(line[:, None] == line[None, :])
        entry = position[first] - position[second] + length - 1
        lookup[axis, entry, rows - 1 - first + second] = 1.0
    return lookup


def remote(source, target, sends, recvs, **where):
    return pltpu.make_async_remote_copy(
        src_ref=source, dst_ref=target, send_sem=sends, recv_sem=recvs, **device(**where)
    )


def heads_kernel(
    size_y, size_z, tokens_in, w_qkv, w_out, bias_x_in, bias_y_in, bias_z_in, lookup_in, result,
    tokens, bias_x, bias_y, bias_z, lookup, in_sem, own_sem, lines, wq, wo, padded, offsets, biases, qkv, mixed, ymixed, back, summed, parts, total,
    up_send, up_recv, down_send, down_recv, side_send, side_recv,
    y_send, y_recv, far_send, far_recv, twin_send, twin_recv, relay_send, relay_recv,
    o_send, o_recv, of_send, of_recv, ry_send, ry_recv, ez_send, ez_recv,
):
    me_y, me_z = lax.axis_index("gy"), lax.axis_index("gz")
    samples, length, rows_z, features = tokens.shape
    rows = length * rows_z
    depth = w_qkv.shape[0]
    wide = 2 * HEAD
    pairs = HEADS // (2 * size_z)
    slots = 3 * pairs
    items = slots + pairs
    levels = size_y // 2
    part_y, part_z = rows // size_y, rows // size_z
    level, side = me_y // 2, lax.rem(me_y, 2)
    core, flank = lax.rem(me_z, 2), me_z // 2
    above, below = {"gy": me_y + 2}, {"gy": me_y - 2}
    beside = {"gy": level * 2 + 1 - side}
    twin = me_z + 1 - 2 * core
    far = me_z + 2 - 4 * flank

    inputs = [
        pltpu.make_async_copy(source, target, in_sem.at[index])
        for index, (source, target) in enumerate(
            (
                (tokens_in, tokens), (bias_x_in, bias_x), (bias_y_in, bias_y),
                (bias_z_in, bias_z), (lookup_in, lookup),
            )
        )
    ]
    for copy in inputs:
        copy.start()

    barrier = pltpu.get_barrier_semaphore()
    for dist in (1, 2):
        pl.when(level + dist < levels)(
            lambda: pl.semaphore_signal(barrier, inc=1, **device(gy=me_y + 2 * dist))
        )
        pl.when(level - dist >= 0)(
            lambda: pl.semaphore_signal(barrier, inc=1, **device(gy=me_y - 2 * dist))
        )
    pl.semaphore_signal(barrier, inc=1, **device(**beside))
    pl.semaphore_signal(barrier, inc=1, **device(gz=twin))
    pl.semaphore_signal(barrier, inc=1, **device(gz=far))
    near = jnp.minimum(level, 2) + jnp.minimum(levels - 1 - level, 2)
    pl.semaphore_wait(barrier, near + 3)

    def item_ref(item):
        return wq.at[item] if item < slots else wo.at[me_z * pairs + item - slots]

    def own_ref(item):
        if item < slots:
            start = item % 3 * features + (me_z * pairs + item // 3) * wide
            return w_qkv.at[:, pl.ds(pl.multiple_of(start, wide), wide)]
        start = (me_z * pairs + item - slots) * wide
        return w_out.at[:, pl.ds(pl.multiple_of(start, wide), wide)]

    def transfer(item, lev, sid, sends, recvs, slot, where, own=False):
        block = item_ref(item).at[pl.ds(pl.multiple_of((lev * 2 + sid) * depth, depth), depth)]
        source = own_ref(item) if own else block
        return remote(source, block, sends.at[item, slot], recvs.at[item, slot], **where)

    def up(item, step, own=False):
        return transfer(item, level - step, side, up_send, up_recv, step, above, own)

    def up_in(item, step):
        return transfer(item, level - 1 - step, side, up_send, up_recv, step, above)

    def down(item, step, own=False):
        return transfer(item, level + step, side, down_send, down_recv, step, below, own)

    def down_in(item, step):
        return transfer(item, level + 1 + step, side, down_send, down_recv, step, below)

    def across(item, lev, own=False):
        return transfer(item, lev, side, side_send, side_recv, lev, beside, own)

    def across_in(item, lev):
        return transfer(item, lev, 1 - side, side_send, side_recv, lev, beside)

    def far_block(item, lev, sid, gz):
        part, index = item - slots, lev * 2 + sid
        ref = wo.at[gz * pairs + part].at[pl.ds(pl.multiple_of(index * depth, depth), depth)]
        return remote(ref, ref, of_send.at[part, index], of_recv.at[part, index], gz=far)

    def block_out(item, lev, sid):
        if item >= slots:
            far_block(item, lev, sid, me_z).start()

    def own_blocks(item):
        pl.when(level + 1 < levels)(lambda: up(item, 0, True).start())
        pl.when(level > 0)(lambda: down(item, 0, True).start())
        across(item, level, True).start()

    def chain(item, step):
        @pl.when(level - 1 - step >= 0)
        def _():
            up_in(item, step).wait_recv()
            pl.when(level + 1 < levels)(lambda: up(item, step + 1).start())
            across(item, level - 1 - step).start()
            block_out(item, level - 1 - step, side)

        @pl.when(level + 1 + step < levels)
        def _():
            down_in(item, step).wait_recv()
            pl.when(level > 0)(lambda: down(item, step + 1).start())
            across(item, level + 1 + step).start()
            block_out(item, level + 1 + step, side)

    def reach(item, dist, rise, passed=False):
        sends, recvs = (up_send, up_recv) if rise else (down_send, down_recv)
        sign = 1 if rise else -1
        if passed:
            return transfer(item, level - 2 * sign, side, sends, recvs, 2, {"gy": me_y + 2 * sign})
        return transfer(
            item, level, side, sends, recvs, dist - 1, {"gy": me_y + 2 * sign * dist}, True
        )

    def direct(item):
        across(item, level, True).start()
        for dist in (1, 2):
            pl.when(level + dist < levels)(lambda: reach(item, dist, True).start())
            pl.when(level - dist >= 0)(lambda: reach(item, dist, False).start())

    def arrive(item, dist):
        @pl.when(level - dist >= 0)
        def _():
            reach(item, dist, True, dist == 3).wait_recv()
            if dist == 2:
                pl.when(level + 1 < levels)(lambda: reach(item, 3, True, True).start())
            across(item, level - dist).start()
            block_out(item, level - dist, side)

        @pl.when(level + dist < levels)
        def _():
            reach(item, dist, False, dist == 3).wait_recv()
            if dist == 2:
                pl.when(level > 0)(lambda: reach(item, 3, False, True).start())
            across(item, level + dist).start()
            block_out(item, level + dist, side)

    def drain_direct(item):
        across(item, level, True).wait_send()
        for dist in range(1, levels):

            @pl.when(level + dist < levels)
            def _():
                if dist < 3:
                    reach(item, dist, True).wait_send()
                across(item, level + dist).wait_send()

            @pl.when(level - dist >= 0)
            def _():
                if dist < 3:
                    reach(item, dist, False).wait_send()
                across(item, level - dist).wait_send()

        pl.when(jnp.logical_and(level >= 2, level + 1 < levels))(
            lambda: reach(item, 3, True, True).wait_send()
        )
        pl.when(jnp.logical_and(level + 2 < levels, level > 0))(
            lambda: reach(item, 3, False, True).wait_send()
        )

    def from_side(item):
        for lev in range(levels):
            across_in(item, lev).wait_recv()
            block_out(item, lev, 1 - side)

    def drain(item):
        pl.when(level + 1 < levels)(lambda: up(item, 0, True).wait_send())
        pl.when(level > 0)(lambda: down(item, 0, True).wait_send())
        across(item, level, True).wait_send()
        for step in range(1, levels):

            @pl.when(level - step >= 0)
            def _():
                pl.when(level + 1 < levels)(lambda: up(item, step).wait_send())
                across(item, level - step).wait_send()

            @pl.when(level + step < levels)
            def _():
                pl.when(level > 0)(lambda: down(item, step).wait_send())
                across(item, level + step).wait_send()

    pieces = samples + size_y

    def piece_of(index, block):
        if index < samples:
            return lines.at[0, block, index]
        peer = lax.rem(me_y + size_y - (index - samples), size_y)
        return lines.at[1, block, :, pl.ds(pl.multiple_of(peer * part_y, part_y), part_y), :]

    def to_far(index, block=me_z):
        ref = piece_of(index, block)
        return remote(ref, ref, far_send.at[index], far_recv.at[index], gz=far)

    def to_twin(index, block=me_z):
        ref = piece_of(index, block)
        return remote(ref, ref, twin_send.at[index], twin_recv.at[index], gz=twin)

    def relay(index, block=far):
        ref = piece_of(index, block)
        return remote(ref, ref, relay_send.at[index], relay_recv.at[index], gz=twin)

    def spread_piece(index):
        to_far(index).start()
        to_twin(index).start()

    def pass_on(index):
        to_far(index, far).wait_recv()
        relay(index).start()

    def exchange(step):
        peer = lax.rem(me_y + step, size_y)
        return remote(
            lines.at[0, me_z, :, pl.ds(pl.multiple_of(peer * part_y, part_y), part_y), :],
            lines.at[1, me_z, :, pl.ds(pl.multiple_of(me_y * part_y, part_y), part_y), :],
            y_send.at[step - 1], y_recv.at[step - 1], gy=peer,
        )

    def exchange_in(step):
        exchange(step).wait_recv()
        spread_piece(samples + step)

    def share_out(slot, part, block):
        ref = wo.at[block * pairs + part]
        return remote(ref, ref, o_send.at[slot, part], o_recv.at[slot, part], gz=twin)

    def share(part):
        from_side(slots + part)
        share_out(0, part, me_z).start()

    def relay_share(part):
        for index in range(size_y):
            pl.when(index != me_y)(lambda: far_block(slots + part, 0, index, far).wait_recv())
        share_out(1, part, far).start()

    def shared(part):
        share_out(0, part, twin).wait_recv()
        share_out(1, part, far).wait_recv()

    def returns(pair, where):
        some = pl.ds(pl.multiple_of(where * 2 * samples, 2 * samples), 2 * samples)
        there = jnp.where(where == flank, 0, 1)
        copies = []
        for step in range(1, size_y):
            peer = lax.rem(me_y + step, size_y)
            copies.append(
                remote(
                    ymixed.at[pair, peer, some], back.at[pair, me_y, some],
                    ry_send.at[pair, there, step - 1], ry_recv.at[pair, there, step - 1], gy=peer,
                )
            )
        return copies

    def give_back(pair, where):
        along_y(pair, where)
        for copy in returns(pair, where):
            copy.start()

    def sum_out(pair, peer, slot):
        return remote(
            summed.at[pair, peer], parts.at[pair, me_z],
            ez_send.at[pair, slot], ez_recv.at[pair, slot], gz=peer,
        )

    def sums_out(pair, where):
        if where is flank:
            return [sum_out(pair, twin, 0)]
        return [sum_out(pair, far, 1), sum_out(pair, far + twin - me_z, 2)]

    row = lax.broadcasted_iota(jnp.int32, (rows, rows), 0)
    col = lax.broadcasted_iota(jnp.int32, (rows, rows), 1)
    lane = lax.broadcasted_iota(jnp.int32, (rows, wide), 1)
    line_of = (
        lambda r: lax.rem(r, rows_z),
        lambda r: lax.rem(r, part_y),
        lambda r: lax.rem(r, part_z) // rows_z,
    )

    def own_copy(item):
        mine = pl.ds(pl.multiple_of(me_y * depth, depth), depth)
        if item >= items:
            block = far * pairs + item - items
            source = w_out.at[:, pl.ds(pl.multiple_of(block * wide, wide), wide)]
            return pltpu.make_async_copy(source, wo.at[block].at[mine], own_sem.at[item])
        return pltpu.make_async_copy(own_ref(item), item_ref(item).at[mine], own_sem.at[item])

    def normalize():
        inputs[0].wait()
        values = tokens[...].astype(jnp.float32).reshape(samples, rows, features)
        center = jnp.mean(values, axis=-1, keepdims=True)
        spread = jnp.mean((values - center) ** 2, axis=-1, keepdims=True)
        lines[0, me_z] = ((values - center) * lax.rsqrt(spread + 1e-05)).astype(jnp.bfloat16)

    def bias_tables():
        for copy in inputs[1:]:
            copy.wait()
        padded[...] = jnp.zeros(padded.shape, jnp.float32)
        for axis, table in enumerate((bias_x, bias_y, bias_z)):
            padded[axis, :, : table.shape[1]] = table[...]
            offsets[axis] = jnp.dot(
                padded[axis], lookup[axis],
                precision=lax.Precision.HIGHEST, preferred_element_type=jnp.float32,
            )

        def fill(head, carry):
            for axis in range(3):
                same = line_of[axis](row) == line_of[axis](col)
                entry = offsets[axis, pl.ds(me_z * 2 * pairs + head, 1), :]
                table = jnp.broadcast_to(entry, (rows, 2 * rows))
                table = pltpu.roll(table, rows + 1, 1, stride=1, stride_axis=0)
                biases[axis, head] = jnp.where(same, table[:, :rows], -1e30)
            return carry

        lax.fori_loop(0, 2 * pairs, fill, 0)

    def project(group, chosen, where):
        blocks = pl.ds(pl.multiple_of(where * 2, 2), 2)
        flat = lines[group, blocks].reshape(2 * samples * rows, features)
        right = jnp.concatenate([wq[item] for item in chosen], axis=1)
        product = jnp.dot(flat, right, preferred_element_type=jnp.float32)
        for place, item in enumerate(chosen):
            piece = product[:, place * wide : (place + 1) * wide]
            if item % 3 == 0:
                piece = piece * HEAD ** (-0.5)
            qkv[group, item, blocks] = piece.astype(jnp.bfloat16).reshape(2, samples, rows, wide)

    def attend(axis, pair, blocks):
        units = [(block, odd) for block in range(len(blocks)) for odd in range(2)]
        scores, expos, totals, outs = {}, {}, {}, {}
        for unit in units:
            block, odd = unit
            query, keys, _ = blocks[block]
            chosen = jnp.where(lane // HEAD == odd, query, 0)
            scores[unit] = lax.dot_general(
                chosen, keys, (((1,), (1,)), ((), ())), preferred_element_type=jnp.float32
            ) + biases[axis, pair * 2 + odd]
        for unit in units:
            expos[unit] = jnp.exp(scores[unit] - jnp.max(scores[unit], axis=-1, keepdims=True))
            totals[unit] = jnp.sum(expos[unit], axis=-1, keepdims=True)
        for unit in units:
            outs[unit] = jnp.dot(
                expos[unit].astype(jnp.bfloat16), blocks[unit[0]][2],
                preferred_element_type=jnp.float32,
            )
        return [
            jnp.where(
                lane < HEAD,
                outs[block, 0] * (1.0 / totals[block, 0]),
                outs[block, 1] * (1.0 / totals[block, 1]),
            ).astype(jnp.bfloat16)
            for block in range(len(blocks))
        ]

    def along_x(pair, where):
        def body(block, carry):
            blocks = [
                [qkv[0, pair * 3 + m, block, sample] for m in range(3)] for sample in range(samples)
            ]
            for sample, out in enumerate(attend(0, pair, blocks)):
                mixed[0, pair, block, sample] = out
            return carry

        lax.fori_loop(where * 2, where * 2 + 2, body, 0)

    def along_z(pair):
        def body(index, carry):
            some = pl.ds(pl.multiple_of(index * part_z, part_z), part_z)
            blocks = [
                [
                    jnp.concatenate(
                        [qkv[0, pair * 3 + m, z, sample, some, :] for z in range(size_z)], axis=0
                    )
                    for m in range(3)
                ]
                for sample in range(samples)
            ]
            for sample, out in enumerate(attend(2, pair, blocks)):
                for z in range(size_z):
                    mixed[1, pair, z, sample, some, :] = out[z * part_z : (z + 1) * part_z]
            return carry

        lax.fori_loop(0, size_z, body, 0)

    def along_y(pair, where):
        def body(block, carry):
            blocks = [
                [qkv[1, pair * 3 + m, block, sample] for m in range(3)] for sample in range(samples)
            ]
            for sample, out in enumerate(attend(1, pair, blocks)):
                for y in range(size_y):
                    ymixed[pair, y, block * samples + sample] = out[y * part_y : (y + 1) * part_y]
            return carry

        lax.fori_loop(where * 2, where * 2 + 2, body, 0)

    def add_up(pair, where):
        def body(block, carry):
            for sample in range(samples):
                there = jnp.concatenate(
                    [back[pair, y, block * samples + sample] for y in range(size_y)], axis=0
                )
                value = mixed[0, pair, block, sample].astype(jnp.float32) + there.astype(jnp.float32)
                value = value + mixed[1, pair, block, sample].astype(jnp.float32)
                summed[pair, block, sample] = value.astype(jnp.bfloat16)
            return carry

        for copy in returns(pair, where):
            copy.wait_recv()
        some = pl.ds(pl.multiple_of(where * 2 * samples, 2 * samples), 2 * samples)
        back[pair, me_y, some] = ymixed[pair, me_y, some]
        lax.fori_loop(where * 2, where * 2 + 2, body, 0)
        for copy in sums_out(pair, where):
            copy.start()
        if where is flank:
            parts[pair, me_z] = summed[pair, me_z]

    def output(pair):
        for where in (1 - flank, flank):
            for copy in sums_out(pair, where):
                copy.wait_recv()
        left = jnp.concatenate(
            [parts[pair, z].reshape(samples * rows, wide) for z in range(size_z)], axis=1
        )
        for block in range(0, features // wide, 2):
            right = jnp.concatenate(
                [
                    jnp.concatenate(
                        [
                            wo[block + n, (z * pairs + pair) * wide : (z * pairs + pair + 1) * wide]
                            for z in range(size_z)
                        ],
                        axis=0,
                    )
                    for n in range(2)
                ],
                axis=1,
            )
            product = jnp.dot(left, right, preferred_element_type=jnp.float32)
            cols = slice(block * wide, (block + 2) * wide)
            if pair > 0:
                product = product + total[:, cols]
            if pair < pairs - 1:
                total[:, cols] = product
            else:
                residual = tokens[:, :, :, cols].astype(jnp.float32).reshape(samples, rows, 2 * wide)
                result[:, :, cols] = (residual + product.reshape(residual.shape)).astype(jnp.bfloat16)

    other = 1 - flank
    straight = ()
    own_rows = pl.ds(pl.multiple_of(me_y * part_y, part_y), part_y)
    hops = levels - 1
    order = [4, 2, 6, 3, 5, 1, 7]

    def run(first, last, *turns):
        for turn in turns:
            for step in range(hops):
                if first <= turn - step < last:
                    chain(turn - step, step)

    for item in range(slots):
        own_blocks(item)
    for item in range(items + pairs):
        own_copy(item).start()
    normalize()
    for sample in range(samples):
        spread_piece(sample)
    lines[1, me_z, :, own_rows, :] = lines[0, me_z, :, own_rows, :]
    bias_tables()
    run(0, slots, 0, 1, 2, 3)
    pass_on(0)
    run(0, slots, 4, 5)
    pass_on(1)
    run(0, slots, 6)
    for step in order[:3]:
        exchange(step).start()
    run(0, slots, 7)
    from_side(0)
    for step in order[3:]:
        exchange(step).start()
    spread_piece(samples)
    for item in range(slots, items):
        own_blocks(item)
    for item in range(items + pairs):
        own_copy(item).wait()
    for item in range(1, 3):
        from_side(item)
    for sample in range(samples):
        to_twin(sample, twin).wait_recv()
        relay(sample).wait_recv()
    project(0, (0, 1, 2), flank)
    exchange_in(order[0])
    project(0, (0, 1, 2), other)
    exchange_in(order[1])
    along_x(0, flank)
    exchange_in(order[2])
    along_x(0, other)
    exchange_in(order[3])
    run(slots, items, slots)
    along_z(0)
    exchange_in(order[4])
    exchange_in(order[5])
    for item in range(3, 6):
        from_side(item)
    run(slots, items, slots + 1)
    project(0, (3, 4, 5), flank)
    exchange_in(order[6])
    run(slots, items, slots + 2)
    pass_on(samples)
    for step in order[:3]:
        pass_on(samples + step)
    for step in range(size_y):
        to_twin(samples + step, twin).wait_recv()
    project(1, (0, 1, 2), flank)
    run(slots, items, slots + 3)
    give_back(0, flank)
    share(0)
    project(1, (3, 4, 5), flank)
    give_back(1, flank)
    share(1)
    for step in order[3:]:
        pass_on(samples + step)
    for step in range(size_y):
        relay(samples + step).wait_recv()
    project(1, (0, 1, 2), other)
    give_back(0, other)
    project(1, (3, 4, 5), other)
    give_back(1, other)
    project(0, (3, 4, 5), other)
    add_up(0, flank)
    add_up(0, other)
    relay_share(0)
    along_x(1, other)
    relay_share(1)
    along_z(1)
    add_up(1, other)
    along_x(1, flank)
    add_up(1, flank)
    shared(0)
    shared(1)
    output(0)
    output(1)
    for item in range(items):
        if item in straight:
            drain_direct(item)
        else:
            drain(item)
    for index in range(pieces):
        to_far(index).wait_send()
        to_twin(index).wait_send()
        relay(index).wait_send()
    for step in range(1, size_y):
        exchange(step).wait_send()
    for part in range(pairs):
        for slot in range(2):
            share_out(slot, part, me_z).wait_send()
        for index in range(size_y):
            pl.when(index != me_y)(lambda: far_block(slots + part, 0, index, me_z).wait_send())
    for pair in range(pairs):
        for where in (other, flank):
            for copy in returns(pair, where) + sums_out(pair, where):
                copy.wait_send()


VMEM = pl.BlockSpec(memory_space=pltpu.VMEM)
DMA = pltpu.SemaphoreType.DMA


def fast_shards(size_y, size_z, tokens, w_qkv, w_out, bias_x, bias_y, bias_z):
    samples, depth, rows_y, rows_z, features = tokens.shape
    rows = depth * rows_y * rows_z
    levels = size_y // 2
    wide = 2 * HEAD
    pairs = HEADS // (2 * size_z)
    items = 4 * pairs
    pieces = samples + size_y
    lengths = [(table.shape[1] + 1) // 2 for table in (bias_x, bias_y, bias_z)]
    width = -(-max(2 * length - 1 for length in lengths) // 128) * 128
    lookup = offset_lookup(line_places(rows, size_y, size_z, rows_z), lengths, rows, width)
    given = (samples, depth, rows_z, features)
    block = (samples, rows, features)
    piled = (pairs, size_z, samples, rows, wide)
    sliced = (pairs, size_y, size_z * samples, rows // size_y, wide)
    result = pl.pallas_call(
        functools.partial(heads_kernel, size_y, size_z),
        out_shape=jax.ShapeDtypeStruct(block, jnp.bfloat16),
        in_specs=[pl.BlockSpec(memory_space=pl.ANY)] * 7,
        out_specs=VMEM,
        scratch_shapes=[
            pltpu.VMEM(given, jnp.bfloat16),
            pltpu.VMEM(bias_x.shape, jnp.float32),
            pltpu.VMEM(bias_y.shape, jnp.float32),
            pltpu.VMEM(bias_z.shape, jnp.float32),
            pltpu.VMEM(lookup.shape, jnp.float32),
            DMA((5,)), DMA((items + pairs,)),
            pltpu.VMEM((2, size_z) + block, jnp.bfloat16),
            pltpu.VMEM((3 * pairs, features, wide), jnp.bfloat16),
            pltpu.VMEM((features // wide, features, wide), jnp.bfloat16),
            pltpu.VMEM((3, HEADS, width), jnp.float32),
            pltpu.VMEM((3, HEADS, 2 * rows), jnp.float32),
            pltpu.VMEM((3, 2 * pairs, rows, rows), jnp.float32),
            pltpu.VMEM((2, 3 * pairs, size_z, samples, rows, wide), jnp.bfloat16),
            pltpu.VMEM((2,) + piled, jnp.bfloat16),
            pltpu.VMEM(sliced, jnp.bfloat16),
            pltpu.VMEM(sliced, jnp.bfloat16),
            pltpu.VMEM(piled, jnp.bfloat16),
            pltpu.VMEM(piled, jnp.bfloat16),
            pltpu.VMEM((samples * rows, features), jnp.float32),
        ]
        + [DMA((items, levels))] * 6
        + [DMA((size_y - 1,))] * 2
        + [DMA((pieces,))] * 6
        + [DMA((2, pairs))] * 2
        + [DMA((pairs, size_y))] * 2
        + [DMA((pairs, 2, size_y - 1))] * 2
        + [DMA((pairs, size_z - 1))] * 2,
        compiler_params=pltpu.CompilerParams(collective_id=0, has_side_effects=True),
    )(tokens.reshape(given), w_qkv, w_out, bias_x, bias_y, bias_z, jnp.asarray(lookup))
    return result.reshape(tokens.shape)


def body_for(size_y, size_z):
    def body(tokens, *parameters):
        _, depth, rows_y, rows_z, features = tokens.shape
        rows = depth * rows_y * rows_z
        fits = size_y == 8 and size_z == 4 and HEADS % (4 * size_z) == 0 and rows == 2 * HEAD
        if fits and rows_y == 1 and rows % (16 * size_y) == 0 and rows % (16 * size_z) == 0:
            return fast_shards(size_y, size_z, tokens, *parameters)
        return shards(tokens, *parameters)

    return body


def solution(mesh):
    placed = (P(None, None, "gy", "gz", None), P("gy", None), P("gy", None), P(), P(), P())
    return jax.shard_map(
        body_for(mesh.shape["gy"], mesh.shape["gz"]),
        mesh=mesh,
        in_specs=placed,
        out_specs=P(None, None, "gy", "gz", None),
        check_vma=False,
    )
```

```python
import functools

import jax
import jax.numpy as jnp
import numpy as np
from jax import lax
from jax.experimental import pallas as pl
from jax.experimental.pallas import tpu as pltpu
from jax.sharding import PartitionSpec as P

HEADS = 16
HEAD = 64


einsum_forms = {
    1: ("bxyzhs,bwyzhs->byzhxw", "byzhxw,bwyzhs->bxyzhs"),
    2: ("bxyzhs,bxwzhs->bxzhyw", "bxzhyw,bxwzhs->bxyzhs"),
    3: ("bxyzhs,bxywhs->bxyhzw", "bxyhzw,bxywhs->bxyzhs"),
}


def norm_rows(tokens):
    values = tokens.astype(jnp.float32)
    center = jnp.mean(values, axis=-1, keepdims=True)
    spread = jnp.mean((values - center) ** 2, axis=-1, keepdims=True)
    return ((values - center) * lax.rsqrt(spread + 1e-05)).astype(jnp.bfloat16)


def rel_bias(table):
    length = (table.shape[1] + 1) // 2
    offsets = (
        lax.broadcasted_iota(jnp.int32, (length, length), 0)
        - lax.broadcasted_iota(jnp.int32, (length, length), 1)
        + length
        - 1
    )
    lookup = (
        offsets[:, :, None] == lax.broadcasted_iota(jnp.int32, (1, 1, 2 * length - 1), 2)
    ).astype(jnp.float32)
    return jnp.einsum("hr,ijr->hij", table, lookup, precision=lax.Precision.HIGHEST)


def attend(qkv, table, axis):
    dims = qkv.shape
    features = dims[-1] // 3
    parts = qkv.reshape(dims[:-1] + (3, HEADS, HEAD))
    query = parts[..., 0, :, :]
    keys = parts[..., 1, :, :]
    values = parts[..., 2, :, :]
    score_form, mix_form = einsum_forms[axis]
    scores = jnp.einsum(score_form, query, keys, preferred_element_type=jnp.float32) * HEAD ** (
        -0.5
    ) + rel_bias(table)
    scores = scores - jnp.max(scores, axis=-1, keepdims=True)
    expo = jnp.exp(scores)
    weights = (expo / jnp.sum(expo, axis=-1, keepdims=True)).astype(jnp.bfloat16)
    mixed = jnp.einsum(mix_form, weights, values, preferred_element_type=jnp.float32)
    return mixed.reshape(dims[:-1] + (features,)).astype(jnp.bfloat16)


def return_y(result):
    return lax.all_to_all(result, "gy", split_axis=2, concat_axis=1, tiled=True)


def return_z(result):
    return lax.all_to_all(result, "gz", split_axis=3, concat_axis=1, tiled=True)


def shards(tokens, w_qkv, w_out, bias_x, bias_y, bias_z):
    samples, depth, rows_y, rows_z, features = tokens.shape
    normed = norm_rows(tokens)
    gathered = lax.all_gather(w_qkv, "gy", axis=0, tiled=True)

    def project(inputs):
        product = jnp.dot(
            inputs.reshape(-1, features), gathered, preferred_element_type=jnp.float32
        )
        return product.astype(jnp.bfloat16).reshape(inputs.shape[:-1] + (3 * features,))

    along_x = attend(project(normed), bias_x, 1)
    along_y = return_y(
        attend(
            project(lax.all_to_all(normed, "gy", split_axis=1, concat_axis=2, tiled=True)),
            bias_y,
            2,
        )
    )
    along_z = return_z(
        attend(
            project(lax.all_to_all(normed, "gz", split_axis=1, concat_axis=3, tiled=True)),
            bias_z,
            3,
        )
    )
    summed = along_x.astype(jnp.float32) + along_y.astype(jnp.float32) + along_z.astype(jnp.float32)
    summed = summed.astype(jnp.bfloat16).reshape(-1, features)
    residual = tokens.reshape(-1, features).astype(jnp.float32)
    result = residual + jnp.dot(
        summed, lax.all_gather(w_out, "gy", axis=0, tiled=True), preferred_element_type=jnp.float32
    )
    return result.astype(jnp.bfloat16).reshape(tokens.shape)


def device(**where):
    return {"device_id": where, "device_id_type": pl.DeviceIdType.MESH}


def line_places(rows, size_y, size_z, rows_z):
    row = np.arange(rows)
    part_y, part_z = rows // size_y, rows // size_z
    return (
        (row // rows_z, row % rows_z),
        (row // part_y, row % part_y),
        (row // part_z * rows_z + row % rows_z, row % part_z // rows_z),
    )


def offset_lookup(places, lengths, rows, width):
    lookup = np.zeros((len(lengths), width, 2 * rows), np.float32)
    for axis, ((position, line), length) in enumerate(zip(places, lengths)):
        first, second = np.nonzero(line[:, None] == line[None, :])
        entry = position[first] - position[second] + length - 1
        lookup[axis, entry, rows - 1 - first + second] = 1.0
    return lookup


def remote(source, target, sends, recvs, **where):
    return pltpu.make_async_remote_copy(
        src_ref=source, dst_ref=target, send_sem=sends, recv_sem=recvs, **device(**where)
    )


def heads_kernel(
    size_y, size_z, tokens_in, w_qkv, w_out, bias_x_in, bias_y_in, bias_z_in, lookup_in, result,
    tokens, bias_x, bias_y, bias_z, lookup, in_sem, own_sem, lines, wq, wo, padded, offsets, biases, qkv, mixed, ymixed, back, summed, parts, total,
    up_send, up_recv, down_send, down_recv, side_send, side_recv,
    y_send, y_recv, far_send, far_recv, twin_send, twin_recv, relay_send, relay_recv,
    o_send, o_recv, of_send, of_recv, ry_send, ry_recv, ez_send, ez_recv,
):
    me_y, me_z = lax.axis_index("gy"), lax.axis_index("gz")
    samples, length, rows_z, features = tokens.shape
    rows = length * rows_z
    depth = w_qkv.shape[0]
    wide = 2 * HEAD
    pairs = HEADS // (2 * size_z)
    slots = 3 * pairs
    items = slots + pairs
    levels = size_y // 2
    part_y, part_z = rows // size_y, rows // size_z
    level, side = me_y // 2, lax.rem(me_y, 2)
    core, flank = lax.rem(me_z, 2), me_z // 2
    above, below = {"gy": me_y + 2}, {"gy": me_y - 2}
    beside = {"gy": level * 2 + 1 - side}
    twin = me_z + 1 - 2 * core
    far = me_z + 2 - 4 * flank

    inputs = [
        pltpu.make_async_copy(source, target, in_sem.at[index])
        for index, (source, target) in enumerate(
            (
                (tokens_in, tokens), (bias_x_in, bias_x), (bias_y_in, bias_y),
                (bias_z_in, bias_z), (lookup_in, lookup),
            )
        )
    ]
    for copy in inputs:
        copy.start()

    barrier = pltpu.get_barrier_semaphore()
    for dist in (1, 2):
        pl.when(level + dist < levels)(
            lambda: pl.semaphore_signal(barrier, inc=1, **device(gy=me_y + 2 * dist))
        )
        pl.when(level - dist >= 0)(
            lambda: pl.semaphore_signal(barrier, inc=1, **device(gy=me_y - 2 * dist))
        )
    pl.semaphore_signal(barrier, inc=1, **device(**beside))
    pl.semaphore_signal(barrier, inc=1, **device(gz=twin))
    pl.semaphore_signal(barrier, inc=1, **device(gz=far))
    near = jnp.minimum(level, 2) + jnp.minimum(levels - 1 - level, 2)
    pl.semaphore_wait(barrier, near + 3)

    def item_ref(item):
        return wq.at[item] if item < slots else wo.at[me_z * pairs + item - slots]

    def own_ref(item):
        if item < slots:
            start = item % 3 * features + (me_z * pairs + item // 3) * wide
            return w_qkv.at[:, pl.ds(pl.multiple_of(start, wide), wide)]
        start = (me_z * pairs + item - slots) * wide
        return w_out.at[:, pl.ds(pl.multiple_of(start, wide), wide)]

    def transfer(item, lev, sid, sends, recvs, slot, where, own=False):
        block = item_ref(item).at[pl.ds(pl.multiple_of((lev * 2 + sid) * depth, depth), depth)]
        source = own_ref(item) if own else block
        return remote(source, block, sends.at[item, slot], recvs.at[item, slot], **where)

    def up(item, step, own=False):
        return transfer(item, level - step, side, up_send, up_recv, step, above, own)

    def up_in(item, step):
        return transfer(item, level - 1 - step, side, up_send, up_recv, step, above)

    def down(item, step, own=False):
        return transfer(item, level + step, side, down_send, down_recv, step, below, own)

    def down_in(item, step):
        return transfer(item, level + 1 + step, side, down_send, down_recv, step, below)

    def across(item, lev, own=False):
        return transfer(item, lev, side, side_send, side_recv, lev, beside, own)

    def across_in(item, lev):
        return transfer(item, lev, 1 - side, side_send, side_recv, lev, beside)

    def far_block(item, lev, sid, gz):
        part, index = item - slots, lev * 2 + sid
        ref = wo.at[gz * pairs + part].at[pl.ds(pl.multiple_of(index * depth, depth), depth)]
        return remote(ref, ref, of_send.at[part, index], of_recv.at[part, index], gz=far)

    def own_blocks(item):
        pl.when(level + 1 < levels)(lambda: up(item, 0, True).start())
        pl.when(level > 0)(lambda: down(item, 0, True).start())
        across(item, level, True).start()

    def chain(item, step):
        @pl.when(level - 1 - step >= 0)
        def _():
            up_in(item, step).wait_recv()
            pl.when(level + 1 < levels)(lambda: up(item, step + 1).start())
            across(item, level - 1 - step).start()

        @pl.when(level + 1 + step < levels)
        def _():
            down_in(item, step).wait_recv()
            pl.when(level > 0)(lambda: down(item, step + 1).start())
            across(item, level + 1 + step).start()

    def reach(item, dist, rise, passed=False):
        sends, recvs = (up_send, up_recv) if rise else (down_send, down_recv)
        sign = 1 if rise else -1
        if passed:
            return transfer(item, level - 2 * sign, side, sends, recvs, 2, {"gy": me_y + 2 * sign})
        return transfer(
            item, level, side, sends, recvs, dist - 1, {"gy": me_y + 2 * sign * dist}, True
        )

    def direct(item):
        across(item, level, True).start()
        for dist in (1, 2):
            pl.when(level + dist < levels)(lambda: reach(item, dist, True).start())
            pl.when(level - dist >= 0)(lambda: reach(item, dist, False).start())

    def arrive(item, dist):
        @pl.when(level - dist >= 0)
        def _():
            reach(item, dist, True, dist == 3).wait_recv()
            if dist == 2:
                pl.when(level + 1 < levels)(lambda: reach(item, 3, True, True).start())
            across(item, level - dist).start()

        @pl.when(level + dist < levels)
        def _():
            reach(item, dist, False, dist == 3).wait_recv()
            if dist == 2:
                pl.when(level > 0)(lambda: reach(item, 3, False, True).start())
            across(item, level + dist).start()

    def drain_direct(item):
        across(item, level, True).wait_send()
        for dist in range(1, levels):

            @pl.when(level + dist < levels)
            def _():
                if dist < 3:
                    reach(item, dist, True).wait_send()
                across(item, level + dist).wait_send()

            @pl.when(level - dist >= 0)
            def _():
                if dist < 3:
                    reach(item, dist, False).wait_send()
                across(item, level - dist).wait_send()

        pl.when(jnp.logical_and(level >= 2, level + 1 < levels))(
            lambda: reach(item, 3, True, True).wait_send()
        )
        pl.when(jnp.logical_and(level + 2 < levels, level > 0))(
            lambda: reach(item, 3, False, True).wait_send()
        )

    def from_side(item):
        for lev in range(levels):
            across_in(item, lev).wait_recv()

    def drain(item):
        pl.when(level + 1 < levels)(lambda: up(item, 0, True).wait_send())
        pl.when(level > 0)(lambda: down(item, 0, True).wait_send())
        across(item, level, True).wait_send()
        for step in range(1, levels):

            @pl.when(level - step >= 0)
            def _():
                pl.when(level + 1 < levels)(lambda: up(item, step).wait_send())
                across(item, level - step).wait_send()

            @pl.when(level + step < levels)
            def _():
                pl.when(level > 0)(lambda: down(item, step).wait_send())
                across(item, level + step).wait_send()

    pieces = samples + size_y

    def piece_of(index, block):
        if index < samples:
            return lines.at[0, block, index]
        peer = lax.rem(me_y + size_y - (index - samples), size_y)
        return lines.at[1, block, :, pl.ds(pl.multiple_of(peer * part_y, part_y), part_y), :]

    def to_far(index, block=me_z):
        ref = piece_of(index, block)
        return remote(ref, ref, far_send.at[index], far_recv.at[index], gz=far)

    def to_twin(index, block=me_z):
        ref = piece_of(index, block)
        return remote(ref, ref, twin_send.at[index], twin_recv.at[index], gz=twin)

    def relay(index, block=far):
        ref = piece_of(index, block)
        return remote(ref, ref, relay_send.at[index], relay_recv.at[index], gz=twin)

    def spread_piece(index):
        to_far(index).start()
        to_twin(index).start()

    def pass_on(index):
        to_far(index, far).wait_recv()
        relay(index).start()

    def exchange(step):
        peer = lax.rem(me_y + step, size_y)
        return remote(
            lines.at[0, me_z, :, pl.ds(pl.multiple_of(peer * part_y, part_y), part_y), :],
            lines.at[1, me_z, :, pl.ds(pl.multiple_of(me_y * part_y, part_y), part_y), :],
            y_send.at[step - 1], y_recv.at[step - 1], gy=peer,
        )

    def exchange_in(step):
        exchange(step).wait_recv()
        spread_piece(samples + step)

    def share_out(slot, part, block):
        ref = wo.at[block * pairs + part]
        return remote(ref, ref, o_send.at[slot, part], o_recv.at[slot, part], gz=twin)

    def share(part):
        from_side(slots + part)
        for index in range(size_y):
            pl.when(index != me_y)(lambda: far_block(slots + part, 0, index, me_z).start())
        share_out(0, part, me_z).start()

    def relay_share(part):
        for index in range(size_y):
            pl.when(index != me_y)(lambda: far_block(slots + part, 0, index, far).wait_recv())
        share_out(1, part, far).start()

    def shared(part):
        share_out(0, part, twin).wait_recv()
        share_out(1, part, far).wait_recv()

    def returns(pair, where):
        some = pl.ds(pl.multiple_of(where * 2 * samples, 2 * samples), 2 * samples)
        there = jnp.where(where == flank, 0, 1)
        copies = []
        for step in range(1, size_y):
            peer = lax.rem(me_y + step, size_y)
            copies.append(
                remote(
                    ymixed.at[pair, peer, some], back.at[pair, me_y, some],
                    ry_send.at[pair, there, step - 1], ry_recv.at[pair, there, step - 1], gy=peer,
                )
            )
        return copies

    def give_back(pair, where):
        along_y(pair, where)
        for copy in returns(pair, where):
            copy.start()

    def sum_out(pair, peer, slot):
        return remote(
            summed.at[pair, peer], parts.at[pair, me_z],
            ez_send.at[pair, slot], ez_recv.at[pair, slot], gz=peer,
        )

    def sums_out(pair, where):
        if where is flank:
            return [sum_out(pair, twin, 0)]
        return [sum_out(pair, far, 1), sum_out(pair, far + twin - me_z, 2)]

    row = lax.broadcasted_iota(jnp.int32, (rows, rows), 0)
    col = lax.broadcasted_iota(jnp.int32, (rows, rows), 1)
    lane = lax.broadcasted_iota(jnp.int32, (rows, wide), 1)
    line_of = (
        lambda r: lax.rem(r, rows_z),
        lambda r: lax.rem(r, part_y),
        lambda r: lax.rem(r, part_z) // rows_z,
    )

    def own_copy(item):
        mine = pl.ds(pl.multiple_of(me_y * depth, depth), depth)
        if item >= items:
            block = far * pairs + item - items
            source = w_out.at[:, pl.ds(pl.multiple_of(block * wide, wide), wide)]
            return pltpu.make_async_copy(source, wo.at[block].at[mine], own_sem.at[item])
        return pltpu.make_async_copy(own_ref(item), item_ref(item).at[mine], own_sem.at[item])

    def normalize():
        inputs[0].wait()
        values = tokens[...].astype(jnp.float32).reshape(samples, rows, features)
        center = jnp.mean(values, axis=-1, keepdims=True)
        spread = jnp.mean((values - center) ** 2, axis=-1, keepdims=True)
        lines[0, me_z] = ((values - center) * lax.rsqrt(spread + 1e-05)).astype(jnp.bfloat16)

    def bias_tables():
        for copy in inputs[1:]:
            copy.wait()
        padded[...] = jnp.zeros(padded.shape, jnp.float32)
        for axis, table in enumerate((bias_x, bias_y, bias_z)):
            padded[axis, :, : table.shape[1]] = table[...]
            offsets[axis] = jnp.dot(
                padded[axis], lookup[axis],
                precision=lax.Precision.HIGHEST, preferred_element_type=jnp.float32,
            )

        def fill(head, carry):
            for axis in range(3):
                same = line_of[axis](row) == line_of[axis](col)
                entry = offsets[axis, pl.ds(me_z * 2 * pairs + head, 1), :]
                table = jnp.broadcast_to(entry, (rows, 2 * rows))
                table = pltpu.roll(table, rows + 1, 1, stride=1, stride_axis=0)
                biases[axis, head] = jnp.where(same, table[:, :rows], -1e30)
            return carry

        lax.fori_loop(0, 2 * pairs, fill, 0)

    def project(group, chosen, where):
        blocks = pl.ds(pl.multiple_of(where * 2, 2), 2)
        flat = lines[group, blocks].reshape(2 * samples * rows, features)
        right = jnp.concatenate([wq[item] for item in chosen], axis=1)
        product = jnp.dot(flat, right, preferred_element_type=jnp.float32)
        for place, item in enumerate(chosen):
            piece = product[:, place * wide : (place + 1) * wide]
            if item % 3 == 0:
                piece = piece * HEAD ** (-0.5)
            qkv[group, item, blocks] = piece.astype(jnp.bfloat16).reshape(2, samples, rows, wide)

    def attend(axis, pair, blocks):
        units = [(block, odd) for block in range(len(blocks)) for odd in range(2)]
        scores, expos, totals, outs = {}, {}, {}, {}
        for unit in units:
            block, odd = unit
            query, keys, _ = blocks[block]
            chosen = jnp.where(lane // HEAD == odd, query, 0)
            scores[unit] = lax.dot_general(
                chosen, keys, (((1,), (1,)), ((), ())), preferred_element_type=jnp.float32
            ) + biases[axis, pair * 2 + odd]
        for unit in units:
            expos[unit] = jnp.exp(scores[unit] - jnp.max(scores[unit], axis=-1, keepdims=True))
            totals[unit] = jnp.sum(expos[unit], axis=-1, keepdims=True)
        for unit in units:
            outs[unit] = jnp.dot(
                expos[unit].astype(jnp.bfloat16), blocks[unit[0]][2],
                preferred_element_type=jnp.float32,
            )
        return [
            jnp.where(
                lane < HEAD,
                outs[block, 0] * (1.0 / totals[block, 0]),
                outs[block, 1] * (1.0 / totals[block, 1]),
            ).astype(jnp.bfloat16)
            for block in range(len(blocks))
        ]

    def along_x(pair, where):
        def body(block, carry):
            blocks = [
                [qkv[0, pair * 3 + m, block, sample] for m in range(3)] for sample in range(samples)
            ]
            for sample, out in enumerate(attend(0, pair, blocks)):
                mixed[0, pair, block, sample] = out
            return carry

        lax.fori_loop(where * 2, where * 2 + 2, body, 0)

    def along_z(pair):
        def body(index, carry):
            some = pl.ds(pl.multiple_of(index * part_z, part_z), part_z)
            blocks = [
                [
                    jnp.concatenate(
                        [qkv[0, pair * 3 + m, z, sample, some, :] for z in range(size_z)], axis=0
                    )
                    for m in range(3)
                ]
                for sample in range(samples)
            ]
            for sample, out in enumerate(attend(2, pair, blocks)):
                for z in range(size_z):
                    mixed[1, pair, z, sample, some, :] = out[z * part_z : (z + 1) * part_z]
            return carry

        lax.fori_loop(0, size_z, body, 0)

    def along_y(pair, where):
        def body(block, carry):
            blocks = [
                [qkv[1, pair * 3 + m, block, sample] for m in range(3)] for sample in range(samples)
            ]
            for sample, out in enumerate(attend(1, pair, blocks)):
                for y in range(size_y):
                    ymixed[pair, y, block * samples + sample] = out[y * part_y : (y + 1) * part_y]
            return carry

        lax.fori_loop(where * 2, where * 2 + 2, body, 0)

    def add_up(pair, where):
        def body(block, carry):
            for sample in range(samples):
                there = jnp.concatenate(
                    [back[pair, y, block * samples + sample] for y in range(size_y)], axis=0
                )
                value = mixed[0, pair, block, sample].astype(jnp.float32) + there.astype(jnp.float32)
                value = value + mixed[1, pair, block, sample].astype(jnp.float32)
                summed[pair, block, sample] = value.astype(jnp.bfloat16)
            return carry

        for copy in returns(pair, where):
            copy.wait_recv()
        some = pl.ds(pl.multiple_of(where * 2 * samples, 2 * samples), 2 * samples)
        back[pair, me_y, some] = ymixed[pair, me_y, some]
        lax.fori_loop(where * 2, where * 2 + 2, body, 0)
        for copy in sums_out(pair, where):
            copy.start()
        if where is flank:
            parts[pair, me_z] = summed[pair, me_z]

    def output(pair):
        for where in (1 - flank, flank):
            for copy in sums_out(pair, where):
                copy.wait_recv()
        left = jnp.concatenate(
            [parts[pair, z].reshape(samples * rows, wide) for z in range(size_z)], axis=1
        )
        for block in range(0, features // wide, 2):
            right = jnp.concatenate(
                [
                    jnp.concatenate(
                        [
                            wo[block + n, (z * pairs + pair) * wide : (z * pairs + pair + 1) * wide]
                            for z in range(size_z)
                        ],
                        axis=0,
                    )
                    for n in range(2)
                ],
                axis=1,
            )
            product = jnp.dot(left, right, preferred_element_type=jnp.float32)
            cols = slice(block * wide, (block + 2) * wide)
            if pair > 0:
                product = product + total[:, cols]
            if pair < pairs - 1:
                total[:, cols] = product
            else:
                residual = tokens[:, :, :, cols].astype(jnp.float32).reshape(samples, rows, 2 * wide)
                result[:, :, cols] = (residual + product.reshape(residual.shape)).astype(jnp.bfloat16)

    other = 1 - flank
    straight = ()
    own_rows = pl.ds(pl.multiple_of(me_y * part_y, part_y), part_y)
    hops = levels - 1
    order = [4, 2, 6, 3, 5, 1, 7]

    def run(first, last, *turns):
        for turn in turns:
            for step in range(hops):
                if first <= turn - step < last:
                    chain(turn - step, step)

    for item in range(slots):
        own_blocks(item)
    for item in range(items + pairs):
        own_copy(item).start()
    normalize()
    for sample in range(samples):
        spread_piece(sample)
    lines[1, me_z, :, own_rows, :] = lines[0, me_z, :, own_rows, :]
    bias_tables()
    run(0, slots, 0, 1, 2, 3)
    pass_on(0)
    run(0, slots, 4, 5)
    pass_on(1)
    run(0, slots, 6)
    for step in order[:3]:
        exchange(step).start()
    run(0, slots, 7)
    for item in range(slots, items):
        own_blocks(item)
    from_side(0)
    for step in order[3:]:
        exchange(step).start()
    spread_piece(samples)
    for item in range(items + pairs):
        own_copy(item).wait()
    for item in range(1, 3):
        from_side(item)
    for sample in range(samples):
        to_twin(sample, twin).wait_recv()
        relay(sample).wait_recv()
    project(0, (0, 1, 2), flank)
    exchange_in(order[0])
    project(0, (0, 1, 2), other)
    exchange_in(order[1])
    along_x(0, flank)
    exchange_in(order[2])
    along_x(0, other)
    exchange_in(order[3])
    run(slots, items, slots)
    along_z(0)
    exchange_in(order[4])
    exchange_in(order[5])
    for item in range(3, 6):
        from_side(item)
    run(slots, items, slots + 1)
    project(0, (3, 4, 5), flank)
    exchange_in(order[6])
    run(slots, items, slots + 2)
    pass_on(samples)
    for step in order[:3]:
        pass_on(samples + step)
    for step in range(size_y):
        to_twin(samples + step, twin).wait_recv()
    project(1, (0, 1, 2), flank)
    run(slots, items, slots + 3)
    give_back(0, flank)
    for step in order[3:]:
        pass_on(samples + step)
    share(0)
    project(1, (3, 4, 5), flank)
    give_back(1, flank)
    share(1)
    for step in range(size_y):
        relay(samples + step).wait_recv()
    project(1, (0, 1, 2), other)
    give_back(0, other)
    project(1, (3, 4, 5), other)
    give_back(1, other)
    project(0, (3, 4, 5), other)
    along_x(1, other)
    add_up(0, flank)
    along_z(1)
    add_up(0, other)
    relay_share(0)
    add_up(1, other)
    along_x(1, flank)
    relay_share(1)
    add_up(1, flank)
    shared(0)
    shared(1)
    output(0)
    output(1)
    for item in range(items):
        if item in straight:
            drain_direct(item)
        else:
            drain(item)
    for index in range(pieces):
        to_far(index).wait_send()
        to_twin(index).wait_send()
        relay(index).wait_send()
    for step in range(1, size_y):
        exchange(step).wait_send()
    for part in range(pairs):
        for slot in range(2):
            share_out(slot, part, me_z).wait_send()
        for index in range(size_y):
            pl.when(index != me_y)(lambda: far_block(slots + part, 0, index, me_z).wait_send())
    for pair in range(pairs):
        for where in (other, flank):
            for copy in returns(pair, where) + sums_out(pair, where):
                copy.wait_send()


VMEM = pl.BlockSpec(memory_space=pltpu.VMEM)
DMA = pltpu.SemaphoreType.DMA


def fast_shards(size_y, size_z, tokens, w_qkv, w_out, bias_x, bias_y, bias_z):
    samples, depth, rows_y, rows_z, features = tokens.shape
    rows = depth * rows_y * rows_z
    levels = size_y // 2
    wide = 2 * HEAD
    pairs = HEADS // (2 * size_z)
    items = 4 * pairs
    pieces = samples + size_y
    lengths = [(table.shape[1] + 1) // 2 for table in (bias_x, bias_y, bias_z)]
    width = -(-max(2 * length - 1 for length in lengths) // 128) * 128
    lookup = offset_lookup(line_places(rows, size_y, size_z, rows_z), lengths, rows, width)
    given = (samples, depth, rows_z, features)
    block = (samples, rows, features)
    piled = (pairs, size_z, samples, rows, wide)
    sliced = (pairs, size_y, size_z * samples, rows // size_y, wide)
    result = pl.pallas_call(
        functools.partial(heads_kernel, size_y, size_z),
        out_shape=jax.ShapeDtypeStruct(block, jnp.bfloat16),
        in_specs=[pl.BlockSpec(memory_space=pl.ANY)] * 7,
        out_specs=VMEM,
        scratch_shapes=[
            pltpu.VMEM(given, jnp.bfloat16),
            pltpu.VMEM(bias_x.shape, jnp.float32),
            pltpu.VMEM(bias_y.shape, jnp.float32),
            pltpu.VMEM(bias_z.shape, jnp.float32),
            pltpu.VMEM(lookup.shape, jnp.float32),
            DMA((5,)), DMA((items + pairs,)),
            pltpu.VMEM((2, size_z) + block, jnp.bfloat16),
            pltpu.VMEM((3 * pairs, features, wide), jnp.bfloat16),
            pltpu.VMEM((features // wide, features, wide), jnp.bfloat16),
            pltpu.VMEM((3, HEADS, width), jnp.float32),
            pltpu.VMEM((3, HEADS, 2 * rows), jnp.float32),
            pltpu.VMEM((3, 2 * pairs, rows, rows), jnp.float32),
            pltpu.VMEM((2, 3 * pairs, size_z, samples, rows, wide), jnp.bfloat16),
            pltpu.VMEM((2,) + piled, jnp.bfloat16),
            pltpu.VMEM(sliced, jnp.bfloat16),
            pltpu.VMEM(sliced, jnp.bfloat16),
            pltpu.VMEM(piled, jnp.bfloat16),
            pltpu.VMEM(piled, jnp.bfloat16),
            pltpu.VMEM((samples * rows, features), jnp.float32),
        ]
        + [DMA((items, levels))] * 6
        + [DMA((size_y - 1,))] * 2
        + [DMA((pieces,))] * 6
        + [DMA((2, pairs))] * 2
        + [DMA((pairs, size_y))] * 2
        + [DMA((pairs, 2, size_y - 1))] * 2
        + [DMA((pairs, size_z - 1))] * 2,
        compiler_params=pltpu.CompilerParams(collective_id=0, has_side_effects=True),
    )(tokens.reshape(given), w_qkv, w_out, bias_x, bias_y, bias_z, jnp.asarray(lookup))
    return result.reshape(tokens.shape)


def body_for(size_y, size_z):
    def body(tokens, *parameters):
        _, depth, rows_y, rows_z, features = tokens.shape
        rows = depth * rows_y * rows_z
        fits = size_y == 8 and size_z == 4 and HEADS % (4 * size_z) == 0 and rows == 2 * HEAD
        if fits and rows_y == 1 and rows % (16 * size_y) == 0 and rows % (16 * size_z) == 0:
            return fast_shards(size_y, size_z, tokens, *parameters)
        return shards(tokens, *parameters)

    return body


def solution(mesh):
    placed = (P(None, None, "gy", "gz", None), P("gy", None), P("gy", None), P(), P(), P())
    return jax.shard_map(
        body_for(mesh.shape["gy"], mesh.shape["gz"]),
        mesh=mesh,
        in_specs=placed,
        out_specs=P(None, None, "gy", "gz", None),
        check_vma=False,
    )
```

```python
import functools

import jax
import jax.numpy as jnp
import numpy as np
from jax import lax
from jax.experimental import pallas as pl
from jax.experimental.pallas import tpu as pltpu
from jax.sharding import PartitionSpec as P

HEADS = 16
HEAD = 64


einsum_forms = {
    1: ("bxyzhs,bwyzhs->byzhxw", "byzhxw,bwyzhs->bxyzhs"),
    2: ("bxyzhs,bxwzhs->bxzhyw", "bxzhyw,bxwzhs->bxyzhs"),
    3: ("bxyzhs,bxywhs->bxyhzw", "bxyhzw,bxywhs->bxyzhs"),
}


def norm_rows(tokens):
    values = tokens.astype(jnp.float32)
    center = jnp.mean(values, axis=-1, keepdims=True)
    spread = jnp.mean((values - center) ** 2, axis=-1, keepdims=True)
    return ((values - center) * lax.rsqrt(spread + 1e-05)).astype(jnp.bfloat16)


def rel_bias(table):
    length = (table.shape[1] + 1) // 2
    offsets = (
        lax.broadcasted_iota(jnp.int32, (length, length), 0)
        - lax.broadcasted_iota(jnp.int32, (length, length), 1)
        + length
        - 1
    )
    lookup = (
        offsets[:, :, None] == lax.broadcasted_iota(jnp.int32, (1, 1, 2 * length - 1), 2)
    ).astype(jnp.float32)
    return jnp.einsum("hr,ijr->hij", table, lookup, precision=lax.Precision.HIGHEST)


def attend(qkv, table, axis):
    dims = qkv.shape
    features = dims[-1] // 3
    parts = qkv.reshape(dims[:-1] + (3, HEADS, HEAD))
    query = parts[..., 0, :, :]
    keys = parts[..., 1, :, :]
    values = parts[..., 2, :, :]
    score_form, mix_form = einsum_forms[axis]
    scores = jnp.einsum(score_form, query, keys, preferred_element_type=jnp.float32) * HEAD ** (
        -0.5
    ) + rel_bias(table)
    scores = scores - jnp.max(scores, axis=-1, keepdims=True)
    expo = jnp.exp(scores)
    weights = (expo / jnp.sum(expo, axis=-1, keepdims=True)).astype(jnp.bfloat16)
    mixed = jnp.einsum(mix_form, weights, values, preferred_element_type=jnp.float32)
    return mixed.reshape(dims[:-1] + (features,)).astype(jnp.bfloat16)


def return_y(result):
    return lax.all_to_all(result, "gy", split_axis=2, concat_axis=1, tiled=True)


def return_z(result):
    return lax.all_to_all(result, "gz", split_axis=3, concat_axis=1, tiled=True)


def shards(tokens, w_qkv, w_out, bias_x, bias_y, bias_z):
    samples, depth, rows_y, rows_z, features = tokens.shape
    normed = norm_rows(tokens)
    gathered = lax.all_gather(w_qkv, "gy", axis=0, tiled=True)

    def project(inputs):
        product = jnp.dot(
            inputs.reshape(-1, features), gathered, preferred_element_type=jnp.float32
        )
        return product.astype(jnp.bfloat16).reshape(inputs.shape[:-1] + (3 * features,))

    along_x = attend(project(normed), bias_x, 1)
    along_y = return_y(
        attend(
            project(lax.all_to_all(normed, "gy", split_axis=1, concat_axis=2, tiled=True)),
            bias_y,
            2,
        )
    )
    along_z = return_z(
        attend(
            project(lax.all_to_all(normed, "gz", split_axis=1, concat_axis=3, tiled=True)),
            bias_z,
            3,
        )
    )
    summed = along_x.astype(jnp.float32) + along_y.astype(jnp.float32) + along_z.astype(jnp.float32)
    summed = summed.astype(jnp.bfloat16).reshape(-1, features)
    residual = tokens.reshape(-1, features).astype(jnp.float32)
    result = residual + jnp.dot(
        summed, lax.all_gather(w_out, "gy", axis=0, tiled=True), preferred_element_type=jnp.float32
    )
    return result.astype(jnp.bfloat16).reshape(tokens.shape)


def device(**where):
    return {"device_id": where, "device_id_type": pl.DeviceIdType.MESH}


def line_places(rows, size_y, size_z, rows_z):
    row = np.arange(rows)
    part_y, part_z = rows // size_y, rows // size_z
    return (
        (row // rows_z, row % rows_z),
        (row // part_y, row % part_y),
        (row // part_z * rows_z + row % rows_z, row % part_z // rows_z),
    )


def offset_lookup(places, lengths, rows, width):
    lookup = np.zeros((len(lengths), width, 2 * rows), np.float32)
    for axis, ((position, line), length) in enumerate(zip(places, lengths)):
        first, second = np.nonzero(line[:, None] == line[None, :])
        entry = position[first] - position[second] + length - 1
        lookup[axis, entry, rows - 1 - first + second] = 1.0
    return lookup


def remote(source, target, sends, recvs, **where):
    return pltpu.make_async_remote_copy(
        src_ref=source, dst_ref=target, send_sem=sends, recv_sem=recvs, **device(**where)
    )


def heads_kernel(
    size_y, size_z, tokens_in, w_qkv, w_out, bias_x_in, bias_y_in, bias_z_in, lookup_in, result,
    tokens, bias_x, bias_y, bias_z, lookup, in_sem, own_sem, lines, wq, wo, padded, offsets, biases, qkv, mixed, ymixed, back, summed, parts, total,
    up_send, up_recv, down_send, down_recv, side_send, side_recv,
    y_send, y_recv, far_send, far_recv, twin_send, twin_recv, relay_send, relay_recv,
    o_send, o_recv, of_send, of_recv, ry_send, ry_recv, ez_send, ez_recv,
):
    me_y, me_z = lax.axis_index("gy"), lax.axis_index("gz")
    samples, length, rows_z, features = tokens.shape
    rows = length * rows_z
    depth = w_qkv.shape[0]
    wide = 2 * HEAD
    pairs = HEADS // (2 * size_z)
    slots = 3 * pairs
    items = slots + pairs
    levels = size_y // 2
    part_y, part_z = rows // size_y, rows // size_z
    level, side = me_y // 2, lax.rem(me_y, 2)
    core, flank = lax.rem(me_z, 2), me_z // 2
    above, below = {"gy": me_y + 2}, {"gy": me_y - 2}
    beside = {"gy": level * 2 + 1 - side}
    twin = me_z + 1 - 2 * core
    far = me_z + 2 - 4 * flank

    inputs = [
        pltpu.make_async_copy(source, target, in_sem.at[index])
        for index, (source, target) in enumerate(
            (
                (tokens_in, tokens), (bias_x_in, bias_x), (bias_y_in, bias_y),
                (bias_z_in, bias_z), (lookup_in, lookup),
            )
        )
    ]
    for copy in inputs:
        copy.start()

    barrier = pltpu.get_barrier_semaphore()
    for dist in (1,):
        pl.when(level + dist < levels)(
            lambda: pl.semaphore_signal(barrier, inc=1, **device(gy=me_y + 2 * dist))
        )
        pl.when(level - dist >= 0)(
            lambda: pl.semaphore_signal(barrier, inc=1, **device(gy=me_y - 2 * dist))
        )
    pl.semaphore_signal(barrier, inc=1, **device(**beside))
    pl.semaphore_signal(barrier, inc=1, **device(gz=twin))
    pl.semaphore_signal(barrier, inc=1, **device(gz=far))
    near = jnp.minimum(level, 1) + jnp.minimum(levels - 1 - level, 1)
    pl.semaphore_wait(barrier, near + 3)

    def item_ref(item):
        return wq.at[item] if item < slots else wo.at[me_z * pairs + item - slots]

    def own_ref(item):
        if item < slots:
            start = item % 3 * features + (me_z * pairs + item // 3) * wide
            return w_qkv.at[:, pl.ds(pl.multiple_of(start, wide), wide)]
        start = (me_z * pairs + item - slots) * wide
        return w_out.at[:, pl.ds(pl.multiple_of(start, wide), wide)]

    def transfer(item, lev, sid, sends, recvs, slot, where, own=False):
        block = item_ref(item).at[pl.ds(pl.multiple_of((lev * 2 + sid) * depth, depth), depth)]
        source = own_ref(item) if own else block
        return remote(source, block, sends.at[item, slot], recvs.at[item, slot], **where)

    def up(item, step, own=False):
        return transfer(item, level - step, side, up_send, up_recv, step, above, own)

    def up_in(item, step):
        return transfer(item, level - 1 - step, side, up_send, up_recv, step, above)

    def down(item, step, own=False):
        return transfer(item, level + step, side, down_send, down_recv, step, below, own)

    def down_in(item, step):
        return transfer(item, level + 1 + step, side, down_send, down_recv, step, below)

    def across(item, lev, own=False):
        return transfer(item, lev, side, side_send, side_recv, lev, beside, own)

    def across_in(item, lev):
        return transfer(item, lev, 1 - side, side_send, side_recv, lev, beside)

    def far_block(item, lev, sid, gz):
        part, index = item - slots, lev * 2 + sid
        ref = wo.at[gz * pairs + part].at[pl.ds(pl.multiple_of(index * depth, depth), depth)]
        return remote(ref, ref, of_send.at[part, index], of_recv.at[part, index], gz=far)

    def own_blocks(item):
        pl.when(level + 1 < levels)(lambda: up(item, 0, True).start())
        pl.when(level > 0)(lambda: down(item, 0, True).start())
        across(item, level, True).start()

    def chain(item, step):
        @pl.when(level - 1 - step >= 0)
        def _():
            up_in(item, step).wait_recv()
            pl.when(level + 1 < levels)(lambda: up(item, step + 1).start())
            across(item, level - 1 - step).start()

        @pl.when(level + 1 + step < levels)
        def _():
            down_in(item, step).wait_recv()
            pl.when(level > 0)(lambda: down(item, step + 1).start())
            across(item, level + 1 + step).start()

    def reach(item, dist, rise, passed=False):
        sends, recvs = (up_send, up_recv) if rise else (down_send, down_recv)
        sign = 1 if rise else -1
        if passed:
            return transfer(item, level - 2 * sign, side, sends, recvs, 2, {"gy": me_y + 2 * sign})
        return transfer(
            item, level, side, sends, recvs, dist - 1, {"gy": me_y + 2 * sign * dist}, True
        )

    def direct(item):
        across(item, level, True).start()
        for dist in (1, 2):
            pl.when(level + dist < levels)(lambda: reach(item, dist, True).start())
            pl.when(level - dist >= 0)(lambda: reach(item, dist, False).start())

    def arrive(item, dist):
        @pl.when(level - dist >= 0)
        def _():
            reach(item, dist, True, dist == 3).wait_recv()
            if dist == 2:
                pl.when(level + 1 < levels)(lambda: reach(item, 3, True, True).start())
            across(item, level - dist).start()

        @pl.when(level + dist < levels)
        def _():
            reach(item, dist, False, dist == 3).wait_recv()
            if dist == 2:
                pl.when(level > 0)(lambda: reach(item, 3, False, True).start())
            across(item, level + dist).start()

    def drain_direct(item):
        across(item, level, True).wait_send()
        for dist in range(1, levels):

            @pl.when(level + dist < levels)
            def _():
                if dist < 3:
                    reach(item, dist, True).wait_send()
                across(item, level + dist).wait_send()

            @pl.when(level - dist >= 0)
            def _():
                if dist < 3:
                    reach(item, dist, False).wait_send()
                across(item, level - dist).wait_send()

        pl.when(jnp.logical_and(level >= 2, level + 1 < levels))(
            lambda: reach(item, 3, True, True).wait_send()
        )
        pl.when(jnp.logical_and(level + 2 < levels, level > 0))(
            lambda: reach(item, 3, False, True).wait_send()
        )

    def from_side(item):
        for lev in range(levels):
            across_in(item, lev).wait_recv()

    def drain(item):
        pl.when(level + 1 < levels)(lambda: up(item, 0, True).wait_send())
        pl.when(level > 0)(lambda: down(item, 0, True).wait_send())
        across(item, level, True).wait_send()
        for step in range(1, levels):

            @pl.when(level - step >= 0)
            def _():
                pl.when(level + 1 < levels)(lambda: up(item, step).wait_send())
                across(item, level - step).wait_send()

            @pl.when(level + step < levels)
            def _():
                pl.when(level > 0)(lambda: down(item, step).wait_send())
                across(item, level + step).wait_send()

    pieces = samples + size_y

    def piece_of(index, block):
        if index < samples:
            return lines.at[0, block, index]
        peer = lax.rem(me_y + size_y - (index - samples), size_y)
        return lines.at[1, block, :, pl.ds(pl.multiple_of(peer * part_y, part_y), part_y), :]

    def to_far(index, block=me_z):
        ref = piece_of(index, block)
        return remote(ref, ref, far_send.at[index], far_recv.at[index], gz=far)

    def to_twin(index, block=me_z):
        ref = piece_of(index, block)
        return remote(ref, ref, twin_send.at[index], twin_recv.at[index], gz=twin)

    def relay(index, block=far):
        ref = piece_of(index, block)
        return remote(ref, ref, relay_send.at[index], relay_recv.at[index], gz=twin)

    def spread_piece(index):
        to_far(index).start()
        to_twin(index).start()

    def pass_on(index):
        to_far(index, far).wait_recv()
        relay(index).start()

    def exchange(step):
        peer = lax.rem(me_y + step, size_y)
        return remote(
            lines.at[0, me_z, :, pl.ds(pl.multiple_of(peer * part_y, part_y), part_y), :],
            lines.at[1, me_z, :, pl.ds(pl.multiple_of(me_y * part_y, part_y), part_y), :],
            y_send.at[step - 1], y_recv.at[step - 1], gy=peer,
        )

    def exchange_in(step):
        exchange(step).wait_recv()
        spread_piece(samples + step)

    def share_out(slot, part, block):
        ref = wo.at[block * pairs + part]
        return remote(ref, ref, o_send.at[slot, part], o_recv.at[slot, part], gz=twin)

    def share(part):
        from_side(slots + part)
        for index in range(size_y):
            pl.when(index != me_y)(lambda: far_block(slots + part, 0, index, me_z).start())
        share_out(0, part, me_z).start()

    def relay_share(part):
        for index in range(size_y):
            pl.when(index != me_y)(lambda: far_block(slots + part, 0, index, far).wait_recv())
        share_out(1, part, far).start()

    def shared(part):
        share_out(0, part, twin).wait_recv()
        share_out(1, part, far).wait_recv()

    def returns(pair, where):
        some = pl.ds(pl.multiple_of(where * 2 * samples, 2 * samples), 2 * samples)
        there = jnp.where(where == flank, 0, 1)
        copies = []
        for step in range(1, size_y):
            peer = lax.rem(me_y + step, size_y)
            copies.append(
                remote(
                    ymixed.at[pair, peer, some], back.at[pair, me_y, some],
                    ry_send.at[pair, there, step - 1], ry_recv.at[pair, there, step - 1], gy=peer,
                )
            )
        return copies

    def give_back(pair, where):
        along_y(pair, where)
        for copy in returns(pair, where):
            copy.start()

    def sum_out(pair, peer, slot):
        return remote(
            summed.at[pair, peer], parts.at[pair, me_z],
            ez_send.at[pair, slot], ez_recv.at[pair, slot], gz=peer,
        )

    def sums_out(pair, where):
        if where is flank:
            return [sum_out(pair, twin, 0)]
        return [sum_out(pair, far, 1), sum_out(pair, far + twin - me_z, 2)]

    row = lax.broadcasted_iota(jnp.int32, (rows, rows), 0)
    col = lax.broadcasted_iota(jnp.int32, (rows, rows), 1)
    lane = lax.broadcasted_iota(jnp.int32, (rows, wide), 1)
    line_of = (
        lambda r: lax.rem(r, rows_z),
        lambda r: lax.rem(r, part_y),
        lambda r: lax.rem(r, part_z) // rows_z,
    )

    def own_copy(item):
        mine = pl.ds(pl.multiple_of(me_y * depth, depth), depth)
        if item >= items:
            block = far * pairs + item - items
            source = w_out.at[:, pl.ds(pl.multiple_of(block * wide, wide), wide)]
            return pltpu.make_async_copy(source, wo.at[block].at[mine], own_sem.at[item])
        return pltpu.make_async_copy(own_ref(item), item_ref(item).at[mine], own_sem.at[item])

    def normalize():
        inputs[0].wait()
        values = tokens[...].astype(jnp.float32).reshape(samples, rows, features)
        center = jnp.mean(values, axis=-1, keepdims=True)
        spread = jnp.mean((values - center) ** 2, axis=-1, keepdims=True)
        lines[0, me_z] = ((values - center) * lax.rsqrt(spread + 1e-05)).astype(jnp.bfloat16)

    def bias_tables():
        for copy in inputs[1:]:
            copy.wait()
        padded[...] = jnp.zeros(padded.shape, jnp.float32)
        for axis, table in enumerate((bias_x, bias_y, bias_z)):
            padded[axis, :, : table.shape[1]] = table[...]
            offsets[axis] = jnp.dot(
                padded[axis], lookup[axis],
                precision=lax.Precision.HIGHEST, preferred_element_type=jnp.float32,
            )

        def fill(head, carry):
            for axis in range(3):
                same = line_of[axis](row) == line_of[axis](col)
                entry = offsets[axis, pl.ds(me_z * 2 * pairs + head, 1), :]
                table = jnp.broadcast_to(entry, (rows, 2 * rows))
                table = pltpu.roll(table, rows + 1, 1, stride=1, stride_axis=0)
                biases[axis, head] = jnp.where(same, table[:, :rows], -1e30)
            return carry

        lax.fori_loop(0, 2 * pairs, fill, 0)

    def project(group, chosen, where):
        blocks = pl.ds(pl.multiple_of(where * 2, 2), 2)
        flat = lines[group, blocks].reshape(2 * samples * rows, features)
        right = jnp.concatenate([wq[item] for item in chosen], axis=1)
        product = jnp.dot(flat, right, preferred_element_type=jnp.float32)
        for place, item in enumerate(chosen):
            piece = product[:, place * wide : (place + 1) * wide]
            if item % 3 == 0:
                piece = piece * HEAD ** (-0.5)
            qkv[group, item, blocks] = piece.astype(jnp.bfloat16).reshape(2, samples, rows, wide)

    def attend(axis, pair, blocks):
        units = [(block, odd) for block in range(len(blocks)) for odd in range(2)]
        scores, expos, totals, outs = {}, {}, {}, {}
        for unit in units:
            block, odd = unit
            query, keys, _ = blocks[block]
            chosen = jnp.where(lane // HEAD == odd, query, 0)
            scores[unit] = lax.dot_general(
                chosen, keys, (((1,), (1,)), ((), ())), preferred_element_type=jnp.float32
            ) + biases[axis, pair * 2 + odd]
        for unit in units:
            expos[unit] = jnp.exp(scores[unit] - jnp.max(scores[unit], axis=-1, keepdims=True))
            totals[unit] = jnp.sum(expos[unit], axis=-1, keepdims=True)
        for unit in units:
            outs[unit] = jnp.dot(
                expos[unit].astype(jnp.bfloat16), blocks[unit[0]][2],
                preferred_element_type=jnp.float32,
            )
        return [
            jnp.where(
                lane < HEAD,
                outs[block, 0] * (1.0 / totals[block, 0]),
                outs[block, 1] * (1.0 / totals[block, 1]),
            ).astype(jnp.bfloat16)
            for block in range(len(blocks))
        ]

    def along_x(pair, where):
        def body(block, carry):
            blocks = [
                [qkv[0, pair * 3 + m, block, sample] for m in range(3)] for sample in range(samples)
            ]
            for sample, out in enumerate(attend(0, pair, blocks)):
                mixed[0, pair, block, sample] = out
            return carry

        lax.fori_loop(where * 2, where * 2 + 2, body, 0)

    def along_z(pair):
        def body(index, carry):
            some = pl.ds(pl.multiple_of(index * part_z, part_z), part_z)
            blocks = [
                [
                    jnp.concatenate(
                        [qkv[0, pair * 3 + m, z, sample, some, :] for z in range(size_z)], axis=0
                    )
                    for m in range(3)
                ]
                for sample in range(samples)
            ]
            for sample, out in enumerate(attend(2, pair, blocks)):
                for z in range(size_z):
                    mixed[1, pair, z, sample, some, :] = out[z * part_z : (z + 1) * part_z]
            return carry

        lax.fori_loop(0, size_z, body, 0)

    def along_y(pair, where):
        def body(block, carry):
            blocks = [
                [qkv[1, pair * 3 + m, block, sample] for m in range(3)] for sample in range(samples)
            ]
            for sample, out in enumerate(attend(1, pair, blocks)):
                for y in range(size_y):
                    ymixed[pair, y, block * samples + sample] = out[y * part_y : (y + 1) * part_y]
            return carry

        lax.fori_loop(where * 2, where * 2 + 2, body, 0)

    def add_up(pair, where):
        def body(block, carry):
            for sample in range(samples):
                there = jnp.concatenate(
                    [back[pair, y, block * samples + sample] for y in range(size_y)], axis=0
                )
                value = mixed[0, pair, block, sample].astype(jnp.float32) + there.astype(jnp.float32)
                value = value + mixed[1, pair, block, sample].astype(jnp.float32)
                summed[pair, block, sample] = value.astype(jnp.bfloat16)
            return carry

        for copy in returns(pair, where):
            copy.wait_recv()
        some = pl.ds(pl.multiple_of(where * 2 * samples, 2 * samples), 2 * samples)
        back[pair, me_y, some] = ymixed[pair, me_y, some]
        lax.fori_loop(where * 2, where * 2 + 2, body, 0)
        for copy in sums_out(pair, where):
            copy.start()
        if where is flank:
            parts[pair, me_z] = summed[pair, me_z]

    def output(pair):
        for where in (1 - flank, flank):
            for copy in sums_out(pair, where):
                copy.wait_recv()
        left = jnp.concatenate(
            [parts[pair, z].reshape(samples * rows, wide) for z in range(size_z)], axis=1
        )
        for block in range(0, features // wide, 2):
            right = jnp.concatenate(
                [
                    jnp.concatenate(
                        [
                            wo[block + n, (z * pairs + pair) * wide : (z * pairs + pair + 1) * wide]
                            for z in range(size_z)
                        ],
                        axis=0,
                    )
                    for n in range(2)
                ],
                axis=1,
            )
            product = jnp.dot(left, right, preferred_element_type=jnp.float32)
            cols = slice(block * wide, (block + 2) * wide)
            if pair > 0:
                product = product + total[:, cols]
            if pair < pairs - 1:
                total[:, cols] = product
            else:
                residual = tokens[:, :, :, cols].astype(jnp.float32).reshape(samples, rows, 2 * wide)
                result[:, :, cols] = (residual + product.reshape(residual.shape)).astype(jnp.bfloat16)

    other = 1 - flank
    straight = ()
    own_rows = pl.ds(pl.multiple_of(me_y * part_y, part_y), part_y)
    hops = levels - 1
    order = [4, 2, 6, 3, 5, 1, 7]

    def run(first, last, *turns):
        for turn in turns:
            for step in range(hops):
                if first <= turn - step < last:
                    chain(turn - step, step)

    for item in range(slots):
        own_blocks(item)
    for item in range(items + pairs):
        own_copy(item).start()
    normalize()
    for sample in range(samples):
        spread_piece(sample)
    lines[1, me_z, :, own_rows, :] = lines[0, me_z, :, own_rows, :]
    bias_tables()
    run(0, slots, 0, 1, 2, 3)
    pass_on(0)
    run(0, slots, 4, 5)
    pass_on(1)
    run(0, slots, 6)
    for step in order[:3]:
        exchange(step).start()
    run(0, slots, 7)
    for item in range(slots, items):
        own_blocks(item)
    from_side(0)
    for step in order[3:]:
        exchange(step).start()
    spread_piece(samples)
    for item in range(items + pairs):
        own_copy(item).wait()
    for item in range(1, 3):
        from_side(item)
    for sample in range(samples):
        to_twin(sample, twin).wait_recv()
        relay(sample).wait_recv()
    project(0, (0, 1, 2), flank)
    exchange_in(order[0])
    project(0, (0, 1, 2), other)
    exchange_in(order[1])
    along_x(0, flank)
    exchange_in(order[2])
    along_x(0, other)
    exchange_in(order[3])
    run(slots, items, slots)
    along_z(0)
    exchange_in(order[4])
    exchange_in(order[5])
    for item in range(3, 6):
        from_side(item)
    run(slots, items, slots + 1)
    project(0, (3, 4, 5), flank)
    exchange_in(order[6])
    run(slots, items, slots + 2)
    pass_on(samples)
    for step in order[:3]:
        pass_on(samples + step)
    for step in range(size_y):
        to_twin(samples + step, twin).wait_recv()
    project(1, (0, 1, 2), flank)
    run(slots, items, slots + 3)
    give_back(0, flank)
    for step in order[3:]:
        pass_on(samples + step)
    share(0)
    project(1, (3, 4, 5), flank)
    give_back(1, flank)
    share(1)
    for step in range(size_y):
        relay(samples + step).wait_recv()
    project(1, (0, 1, 2), other)
    give_back(0, other)
    project(1, (3, 4, 5), other)
    give_back(1, other)
    project(0, (3, 4, 5), other)
    along_x(1, other)
    add_up(0, flank)
    along_z(1)
    add_up(0, other)
    relay_share(0)
    add_up(1, other)
    relay_share(1)
    along_x(1, flank)
    add_up(1, flank)
    shared(0)
    shared(1)
    output(0)
    output(1)
    for item in range(items):
        if item in straight:
            drain_direct(item)
        else:
            drain(item)
    for index in range(pieces):
        to_far(index).wait_send()
        to_twin(index).wait_send()
        relay(index).wait_send()
    for step in range(1, size_y):
        exchange(step).wait_send()
    for part in range(pairs):
        for slot in range(2):
            share_out(slot, part, me_z).wait_send()
        for index in range(size_y):
            pl.when(index != me_y)(lambda: far_block(slots + part, 0, index, me_z).wait_send())
    for pair in range(pairs):
        for where in (other, flank):
            for copy in returns(pair, where) + sums_out(pair, where):
                copy.wait_send()


VMEM = pl.BlockSpec(memory_space=pltpu.VMEM)
DMA = pltpu.SemaphoreType.DMA


def fast_shards(size_y, size_z, tokens, w_qkv, w_out, bias_x, bias_y, bias_z):
    samples, depth, rows_y, rows_z, features = tokens.shape
    rows = depth * rows_y * rows_z
    levels = size_y // 2
    wide = 2 * HEAD
    pairs = HEADS // (2 * size_z)
    items = 4 * pairs
    pieces = samples + size_y
    lengths = [(table.shape[1] + 1) // 2 for table in (bias_x, bias_y, bias_z)]
    width = -(-max(2 * length - 1 for length in lengths) // 128) * 128
    lookup = offset_lookup(line_places(rows, size_y, size_z, rows_z), lengths, rows, width)
    given = (samples, depth, rows_z, features)
    block = (samples, rows, features)
    piled = (pairs, size_z, samples, rows, wide)
    sliced = (pairs, size_y, size_z * samples, rows // size_y, wide)
    result = pl.pallas_call(
        functools.partial(heads_kernel, size_y, size_z),
        out_shape=jax.ShapeDtypeStruct(block, jnp.bfloat16),
        in_specs=[pl.BlockSpec(memory_space=pl.ANY)] * 7,
        out_specs=VMEM,
        scratch_shapes=[
            pltpu.VMEM(given, jnp.bfloat16),
            pltpu.VMEM(bias_x.shape, jnp.float32),
            pltpu.VMEM(bias_y.shape, jnp.float32),
            pltpu.VMEM(bias_z.shape, jnp.float32),
            pltpu.VMEM(lookup.shape, jnp.float32),
            DMA((5,)), DMA((items + pairs,)),
            pltpu.VMEM((2, size_z) + block, jnp.bfloat16),
            pltpu.VMEM((3 * pairs, features, wide), jnp.bfloat16),
            pltpu.VMEM((features // wide, features, wide), jnp.bfloat16),
            pltpu.VMEM((3, HEADS, width), jnp.float32),
            pltpu.VMEM((3, HEADS, 2 * rows), jnp.float32),
            pltpu.VMEM((3, 2 * pairs, rows, rows), jnp.float32),
            pltpu.VMEM((2, 3 * pairs, size_z, samples, rows, wide), jnp.bfloat16),
            pltpu.VMEM((2,) + piled, jnp.bfloat16),
            pltpu.VMEM(sliced, jnp.bfloat16),
            pltpu.VMEM(sliced, jnp.bfloat16),
            pltpu.VMEM(piled, jnp.bfloat16),
            pltpu.VMEM(piled, jnp.bfloat16),
            pltpu.VMEM((samples * rows, features), jnp.float32),
        ]
        + [DMA((items, levels))] * 6
        + [DMA((size_y - 1,))] * 2
        + [DMA((pieces,))] * 6
        + [DMA((2, pairs))] * 2
        + [DMA((pairs, size_y))] * 2
        + [DMA((pairs, 2, size_y - 1))] * 2
        + [DMA((pairs, size_z - 1))] * 2,
        compiler_params=pltpu.CompilerParams(collective_id=0, has_side_effects=True),
    )(tokens.reshape(given), w_qkv, w_out, bias_x, bias_y, bias_z, jnp.asarray(lookup))
    return result.reshape(tokens.shape)


def body_for(size_y, size_z):
    def body(tokens, *parameters):
        _, depth, rows_y, rows_z, features = tokens.shape
        rows = depth * rows_y * rows_z
        fits = size_y == 8 and size_z == 4 and HEADS % (4 * size_z) == 0 and rows == 2 * HEAD
        if fits and rows_y == 1 and rows % (16 * size_y) == 0 and rows % (16 * size_z) == 0:
            return fast_shards(size_y, size_z, tokens, *parameters)
        return shards(tokens, *parameters)

    return body


def solution(mesh):
    placed = (P(None, None, "gy", "gz", None), P("gy", None), P("gy", None), P(), P(), P())
    return jax.shard_map(
        body_for(mesh.shape["gy"], mesh.shape["gz"]),
        mesh=mesh,
        in_specs=placed,
        out_specs=P(None, None, "gy", "gz", None),
        check_vma=False,
    )
```
